512 devices in a mesh: grp: 2 (over y), leaf: 32 (over z, core), sub: 8 (over x).
Axes of the slice: x: 8, y: 2, z: 16, core: 2. Of those that a mesh axis runs over, the one named last changes fastest.
The devices are a block of a 8x8x16 slice.
Arguments:
- targets: bfloat16 [64, 1048576], P(None, ('grp', 'leaf', 'sub')), parts along dimension 1, may hold values from -6 to 6
- tree_order: int32 [512, 2048], P(('grp', 'leaf', 'sub')), parts along dimension 0, may hold values from 0 to 2047, each once within a row
- leaf_inverse: bfloat16 [2048, 512, 512], P(('grp', 'leaf', 'sub')), parts along dimension 0, as said below
- cluster_basis: bfloat16 [10, 32, 1048576], P(None, None, ('grp', 'leaf', 'sub')), parts along dimension 2, may hold values from -1.5 to 1.5
- coupling: float32 [512, 10, 32, 64], P(('grp', 'leaf', 'sub')), parts along dimension 0, may hold values from -0.75 to 0.75
- train_coords: bfloat16 [3, 1048576], P(None, ('grp', 'leaf', 'sub')), parts along dimension 1, may hold values from 0 to 1
- test_coords: bfloat16 [3, 1048576], P(None, ('grp', 'leaf', 'sub')), parts along dimension 1, may hold values from 0 to 1
- test_basis: bfloat16 [8, 32, 1048576], P(None, None, ('grp', 'leaf', 'sub')), parts along dimension 2, may hold values from -2.4 to 2.4
- near_leaves: int32 [512, 8], P(('grp', 'leaf', 'sub')), parts along dimension 0, may hold values from 0 to 1023, as said below
Outputs:
- posterior_mean: bfloat16 [64, 1048576], P(None, ('grp', 'leaf', 'sub')), parts along dimension 1
The draws below stay inside these ranges and needn't reach their ends.
There are 2 independent parts, one for each index of `grp`. The reference program is written for one: setup_inputs(seed, part) draws one part's arguments, and reference() takes and returns one part's arrays. A program takes and returns all parts, laid end to end along the dimension named above; each array names one. Nothing has to cross between parts.
Inputs may be any that keep to these rules, and one draw needn't show every extreme that they name: `tree_order`: row d is a permutation of the positions 0 to 2047 within panel d. `near_leaves`: row d names 8 different training leaves, all held by panels d - 1, d or d + 1. `leaf_inverse`: each block is the identity plus dense full-rank entries of spread 0.5 / sqrt(512).
All inputs are finite; a program needn't handle non-finite values.
Results may differ from the reference program's by a relative error of at most 0.0035.
Values may be sent and summed in bfloat16 or wider, within the bound.
No kernel may reach another device: no remote copies, remote signals or barrier semaphores. Data moves between devices by JAX's collectives and lax.ppermute only.
A program may use at most 64 MiB of HBM per device.

```python
import math
import jax
import jax.numpy as jnp
from jax import lax

RHS = 64
LEAF = 512
RANK = 32
NEAR = 8
LEAF_DEV = 4
TEST_DEV = 2048
GROUP_DEVS = 256
PTS_DEV = 2048
NTRAIN = 524288
LEAVES = 1024
NTEST = 524288
LOCAL_LEVELS = 2
DEV_LEVELS = 8
LEVELS = 10


def draw_leaf_inverse(key, part):
    noise = jax.random.normal(jax.random.fold_in(key, 11), (LEAVES, LEAF, LEAF), jnp.float32)
    identity = jnp.eye(LEAF, dtype=jnp.float32)[None]
    return (identity + noise * (0.5 / math.sqrt(LEAF))).astype(jnp.bfloat16)


def draw_test_basis(key, part):
    levels = jnp.arange(DEV_LEVELS, dtype=jnp.float32)
    spread = 0.05 * 8.0 ** (levels / (DEV_LEVELS - 1))
    noise = jnp.clip(jax.random.normal(jax.random.fold_in(key, 23), (DEV_LEVELS, RANK, NTEST), jnp.float32), -6.0, 6.0)
    return (noise * spread[:, None, None]).astype(jnp.bfloat16)


def draw_near_leaves(key, part):
    window = 3 * LEAF_DEV
    device_ids = jnp.arange(GROUP_DEVS, dtype=jnp.int32)[:, None]
    candidates = jnp.arange(window, dtype=jnp.int32)[None, :]
    leaf_ids = (device_ids - 1) * LEAF_DEV + candidates
    valid = (leaf_ids >= 0) & (leaf_ids < LEAVES)
    scores = jax.random.randint(jax.random.fold_in(key, 7), (GROUP_DEVS, window), 0, 1 << 20, dtype=jnp.int32) * window + candidates
    scores = jnp.where(valid, scores, -1)
    chosen = lax.top_k(scores, NEAR)[1].astype(jnp.int32)
    return jnp.take_along_axis(leaf_ids, chosen, axis=1).astype(jnp.int32)


def level_of(key, shape, split, low, high):
    factor_of = 1.0
    for position, blocks in split:
        heights = jax.random.uniform(jax.random.fold_in(jax.random.fold_in(key, 6), position), (blocks,), jnp.float32, low / len(split), high / len(split))
        factor_of = factor_of * jnp.repeat(jnp.exp(heights), shape[position] // blocks).reshape((-1,) + (1,) * (len(shape) - 1 - position))
    return factor_of


def scatter_about(rng, extent, deviation, most, cuts=(), kind=jnp.bfloat16):
    entries = jax.random.normal(rng, extent, jnp.float32) * deviation
    if len(cuts) > 0:
        entries = level_of(rng, extent, cuts, -0.22, 0.18) * entries
    return jnp.clip(entries, min=-most, max=most).astype(kind)


def setup_inputs(seed: int = 0, part: int = 0) -> dict:
    key_of = jax.random.split(jax.random.key(seed), 10)
    part_splits = jax.random.split(jax.random.fold_in(key_of[9], part), 10)
    return {
        "targets": scatter_about(part_splits[0], (RHS, NTRAIN), 1.0, 6.0, ((1, 256),)),
        "tree_order": jax.vmap(lambda own: jax.random.permutation(own, PTS_DEV))(jax.random.split(part_splits[1], GROUP_DEVS)).reshape((GROUP_DEVS, PTS_DEV)).astype(jnp.int32),
        "leaf_inverse": draw_leaf_inverse(jax.random.fold_in(jax.random.fold_in(key_of[9], part), 71), part),
        "cluster_basis": scatter_about(part_splits[3], (LEVELS, RANK, NTRAIN), 0.25, 1.5, ((2, 256),)),
        "coupling": scatter_about(part_splits[4], (GROUP_DEVS, LEVELS, RANK, 2 * RANK), (2 * RANK) ** -0.5, 0.75, ((0, 256),), jnp.float32),
        "train_coords": jnp.clip(1.0 * jax.random.uniform(part_splits[5], (3, NTRAIN), jnp.float32) ** level_of(part_splits[5], (3, NTRAIN), ((1, 256),), -0.2, 0.2), 0.0, 1.0).astype(jnp.bfloat16),
        "test_coords": jnp.clip(1.0 * jax.random.uniform(part_splits[6], (3, NTEST), jnp.float32) ** level_of(part_splits[6], (3, NTEST), ((1, 256),), -0.2, 0.2), 0.0, 1.0).astype(jnp.bfloat16),
        "test_basis": draw_test_basis(jax.random.fold_in(jax.random.fold_in(key_of[9], part), 71), part),
        "near_leaves": draw_near_leaves(jax.random.fold_in(jax.random.fold_in(key_of[9], part), 71), part),
    }


variance = 2.0
length_scale = 0.5
highest = lax.Precision.HIGHEST

def matern(train_pos, test_pos):
    train_f32 = train_pos.astype(jnp.float32)
    test_f32 = test_pos.astype(jnp.float32)
    squared = jnp.zeros((train_f32.shape[1], test_f32.shape[1]), jnp.float32)
    for axis_number in range(3):
        offset = train_f32[axis_number][:, None] - test_f32[axis_number][None, :]
        squared = squared + offset * offset
    scaled = jnp.sqrt(3.0 * squared) / length_scale
    return (variance * (1.0 + scaled) * jnp.exp(-scaled)).astype(jnp.bfloat16)

def reference(targets, tree_order, leaf_inverse, cluster_basis, coupling, train_coords, test_coords, test_basis, near_leaves):
    device_base = (jnp.arange(GROUP_DEVS, dtype=jnp.int32) * PTS_DEV)[:, None]
    flat_index = (tree_order + device_base).reshape(-1).astype(jnp.int32)
    reordered = jnp.take(targets, flat_index, axis=1)

    def solve_panel(pair):
        inverse_part, target_part = pair
        return jnp.einsum('jpq,rjq->rjp', inverse_part.astype(jnp.float32), target_part.astype(jnp.float32), precision=highest)
    inverse_groups = leaf_inverse.reshape(GROUP_DEVS, LEAF_DEV, LEAF, LEAF)
    target_groups = reordered.reshape(RHS, GROUP_DEVS, LEAF_DEV, LEAF).transpose(1, 0, 2, 3)
    solved = lax.map(solve_panel, (inverse_groups, target_groups))
    state = solved.transpose(1, 0, 2, 3).reshape(RHS, NTRAIN)
    for level_index in range(LEVELS):
        child = LEAF * 2 ** level_index
        child_count = NTRAIN // child
        unit = min(child, PTS_DEV)
        unit_count = NTRAIN // unit
        level_basis = cluster_basis[level_index].astype(jnp.float32)
        coefficient = jnp.einsum('kcp,rcp->ckr', level_basis.reshape(RANK, child_count, child), state.reshape(RHS, child_count, child), precision=highest) / math.sqrt(child)
        paired = coefficient.reshape(child_count // 2, 2, RANK, RHS)
        sibling = paired[:, ::-1].reshape(child_count, RANK, RHS)
        joined = jnp.concatenate([coefficient, sibling], axis=1)
        per_unit = jnp.repeat(joined, child // unit, axis=0)
        unit_coupling = jnp.repeat(coupling[:, level_index], PTS_DEV // unit, axis=0)
        mixed = jnp.einsum('uks,usr->ukr', unit_coupling, per_unit, precision=highest)
        update = jnp.einsum('ukr,kup->rup', mixed, level_basis.reshape(RANK, unit_count, unit), precision=highest)
        state = (state.reshape(RHS, unit_count, unit) - update).reshape(RHS, NTRAIN)
    weights = state.astype(jnp.bfloat16)
    weight_leaves = weights.reshape(RHS, LEAVES, LEAF)
    coord_leaves = train_coords.reshape(3, LEAVES, LEAF)
    test_groups = test_coords.reshape(3, GROUP_DEVS, TEST_DEV).transpose(1, 0, 2)

    def near_panel(pair):
        leaf_ids, test_pos = pair
        total = jnp.zeros((RHS, TEST_DEV), jnp.float32)
        for slot_index in range(NEAR):
            leaf_id = leaf_ids[slot_index].astype(jnp.int32)
            train_pos = lax.dynamic_index_in_dim(coord_leaves, leaf_id, 1, keepdims=False)
            leaf_weights = lax.dynamic_index_in_dim(weight_leaves, leaf_id, 1, keepdims=False)
            kernel = matern(train_pos, test_pos)
            total = total + jnp.dot(leaf_weights, kernel, preferred_element_type=jnp.float32)
        return total
    near_sum = lax.map(near_panel, (near_leaves, test_groups))
    far = jnp.zeros((RHS, GROUP_DEVS, TEST_DEV), jnp.float32)
    test_levels = test_basis.reshape(DEV_LEVELS, RANK, GROUP_DEVS, TEST_DEV)
    panel_weights = weights.reshape(RHS, GROUP_DEVS, PTS_DEV).astype(jnp.float32)
    for level_index in range(DEV_LEVELS):
        span = 2 ** level_index
        level_basis = cluster_basis[LOCAL_LEVELS + level_index].reshape(RANK, GROUP_DEVS, PTS_DEV).astype(jnp.float32)
        terms = jnp.einsum('kdp,rdp->dkr', level_basis, panel_weights, precision=highest) / math.sqrt(PTS_DEV * span)
        subtree = terms.reshape(GROUP_DEVS // span, span, RANK, RHS).sum(axis=1)
        sibling_ids = (jnp.arange(GROUP_DEVS, dtype=jnp.int32) // span ^ 1).astype(jnp.int32)
        sibling = jnp.take(subtree, sibling_ids, axis=0)
        far = far + jnp.einsum('dkr,kdt->rdt', sibling, test_levels[level_index].astype(jnp.float32), precision=highest)
    mean = near_sum.transpose(1, 0, 2) / math.sqrt(NEAR * LEAF) + far
    return mean.reshape(RHS, NTEST).astype(jnp.bfloat16)
```

```python
import math

import jax
import jax.numpy as jnp
from jax import lax
from jax.experimental import pallas as pl
from jax.experimental.pallas import tpu as pltpu
from jax.sharding import Mesh
from jax.sharding import PartitionSpec as P

length_scale = 0.5
highest = lax.Precision.HIGHEST
low_axes = ("core", "sub")
panel_axes = ("z", "core", "sub")
f32 = jnp.float32
bf16 = jnp.bfloat16
rows_by_columns = (((1,), (0,)), ((), ()))
rows_by_rows = (((1,), (1,)), ((), ()))
columns_by_columns = (((0,), (0,)), ((), ()))


def thirds(value):
    high = value.astype(bf16)
    rest = value - high.astype(f32)
    middle = rest.astype(bf16)
    low = (rest - middle.astype(f32)).astype(bf16)
    return high, middle, low


def wide_dot(left, right, dims):
    rows = left.shape[0]
    stacked = jnp.concatenate(thirds(left), axis=0)
    product = lax.dot_general(stacked, right, dims, preferred_element_type=f32)
    return product[:rows] + product[rows : 2 * rows] + product[2 * rows :]


def full_dot(left, right, dims=rows_by_columns):
    return lax.dot_general(left, right, dims, precision=highest, preferred_element_type=f32)


def whole_call(body, out_shape, name, scalars=0, scratch=()):
    def call(*operands):
        specs = [
            pl.BlockSpec(memory_space=pltpu.SMEM if i < scalars else pltpu.VMEM)
            for i in range(len(operands))
        ]
        single = not isinstance(out_shape, (list, tuple))
        out_specs = pl.BlockSpec(memory_space=pltpu.VMEM)
        return pl.pallas_call(
            body,
            out_shape=out_shape,
            in_specs=specs,
            out_specs=out_specs if single else [out_specs] * len(out_shape),
            scratch_shapes=list(scratch),
            name=name,
        )(*operands)

    return call


def points_body(train_ref, test_ref, left_ref, right_ref, rows_ref, *, scale):
    dims, count = train_ref.shape
    ones = jnp.ones((1, count), f32)
    for ref, out_ref in ((train_ref, left_ref), (test_ref, right_ref)):
        exact = ref[...].astype(f32)
        norms = scale * jnp.sum(exact * exact, axis=0, keepdims=True)
        norms = [piece.astype(f32) for piece in thirds(norms)]
        if out_ref is left_ref:
            rows = [exact[axis : axis + 1] for axis in range(dims)] * 3 + norms + [ones] * 3
        else:
            pieces = [piece.astype(f32) for piece in thirds(-2.0 * scale * exact)]
            rows = [piece[axis : axis + 1] for piece in pieces for axis in range(dims)]
            rows = rows + [ones] * 3 + norms
        rows_ref[...] = jnp.zeros_like(rows_ref)
        for place, row in enumerate(rows):
            rows_ref[place : place + 1, :] = row
        out_ref[...] = rows_ref[...].astype(bf16)


def mixer_body(basis_ref, coupling_ref, out_ref, *, local_levels, part):
    rank = coupling_ref.shape[1]
    width = basis_ref.shape[0] - local_levels * rank
    points = basis_ref.shape[1]
    basis = basis_ref[local_levels * rank :, :]
    gram = lax.dot_general(basis, basis, rows_by_rows, preferred_element_type=f32)
    level = lax.broadcasted_iota(jnp.int32, (1, width), 1) // rank
    gram = gram * (lax.exp2(-0.5 * level.astype(f32)) / math.sqrt(points))
    for depth in range(width // rank):
        piece = gram[depth * rank : (depth + 1) * rank, :]
        product = full_dot(coupling_ref[local_levels + depth], piece, columns_by_columns)
        for half in range(2):
            for block in range(rank // part):
                start = half * rank + block * part
                out_ref[depth * (rank // part) + block, half * part : (half + 1) * part, :] = (
                    product[start : start + part, :]
                )


def local_body(targets_ref, order_ref, inverse_ref, basis_ref, coupling_ref, state_ref, terms_ref):
    columns, points = targets_ref.shape
    leaf_count, leaf_size, _ = inverse_ref.shape
    rank = coupling_ref.shape[1]
    local_levels = leaf_count.bit_length() - 1
    place = lax.broadcasted_iota(jnp.int32, (points, leaf_size), 0)
    for leaf in range(leaf_count):
        lanes = slice(leaf * leaf_size, (leaf + 1) * leaf_size)
        chosen = jnp.where(place == order_ref[:, lanes], 1.0, 0.0).astype(bf16)
        block = jnp.dot(targets_ref[...], chosen, preferred_element_type=f32).astype(bf16)
        state_ref[:, lanes] = lax.dot_general(
            block, inverse_ref[leaf], rows_by_rows, preferred_element_type=f32
        )
    for level in range(local_levels):
        child = leaf_size << level
        count = points // child
        mixers = coupling_ref[level]
        bases = [
            basis_ref[level * rank : (level + 1) * rank, c * child : (c + 1) * child]
            for c in range(count)
        ]
        sums = [
            wide_dot(state_ref[:, c * child : (c + 1) * child], bases[c], rows_by_rows)
            / math.sqrt(child)
            for c in range(count)
        ]
        for c in range(count):
            joined = jnp.concatenate([sums[c], sums[c ^ 1]], axis=1)
            mixed = full_dot(joined, mixers, rows_by_rows)
            lanes = slice(c * child, (c + 1) * child)
            state_ref[:, lanes] = state_ref[:, lanes] - wide_dot(mixed, bases[c], rows_by_columns)
    width = terms_ref.shape[1]
    level = lax.broadcasted_iota(jnp.int32, (1, width), 1) // rank
    scale = lax.exp2(-0.5 * level.astype(f32)) / math.sqrt(points)
    terms_ref[...] = (
        wide_dot(state_ref[...], basis_ref[local_levels * rank :, :], rows_by_rows) * scale
    )


def distance_body(slots_ref, window_ref, test_ref, out_ref):
    leaf = slots_ref[pl.program_id(0)]
    train = window_ref[leaf]
    step = 256
    for start in range(0, test_ref.shape[1], step):
        squared = lax.dot_general(
            train, test_ref[:, start : start + step], columns_by_columns,
            preferred_element_type=f32,
        )
        squared = jnp.maximum(squared, 1e-20)
        scaled = squared * lax.rsqrt(squared)
        out_ref[0, :, start : start + step] = ((1.0 + scaled) * jnp.exp(-scaled)).astype(bf16)


def distance_kernel(slots, window, test_features, name):
    leaves, rows, leaf_size = window.shape
    tests = test_features.shape[1]
    return pl.pallas_call(
        distance_body,
        out_shape=jax.ShapeDtypeStruct((slots.shape[0], leaf_size, tests), bf16),
        grid_spec=pltpu.PrefetchScalarGridSpec(
            num_scalar_prefetch=1,
            grid=(slots.shape[0],),
            in_specs=[
                pl.BlockSpec((leaves, rows, leaf_size), lambda i, s: (0, 0, 0)),
                pl.BlockSpec(test_features.shape, lambda i, s: (0, 0)),
            ],
            out_specs=pl.BlockSpec((1, leaf_size, tests), lambda i, s: (i, 0, 0)),
        ),
        name=name,
    )(slots, window, test_features)


def node_sums(members, levels):
    sums = [members]
    for _ in range(levels):
        last = sums[-1]
        sums.append([last[i] + last[i + 1] for i in range(0, len(last), 2)])
    return sums


def chain_sums(values, position, levels):
    tree = node_sums(values, levels)
    own, sibling = [], []
    for level in range(levels):
        nodes = tree[level]
        mine = position >> level
        first, second = nodes[0], nodes[1]
        for node in range(2, len(nodes), 2):
            here = (mine >> 1) == (node >> 1)
            first = jnp.where(here, nodes[node], first)
            second = jnp.where(here, nodes[node + 1], second)
        right = (mine & 1) == 1
        own.append(jnp.where(right, second, first))
        sibling.append(jnp.where(right, first, second))
    return own, sibling


def operator_body(place_ref, spread_ref, high_ref, out_ref, *, rank):
    low_count, rows, width = spread_ref.shape
    part = rows // 2
    high_count, _, high_width = high_ref.shape
    low_width = width - high_width
    low_levels = low_count.bit_length() - 1
    high_levels = high_count.bit_length() - 1
    row_level = place_ref[0] * part // rank
    lane_level = lax.broadcasted_iota(jnp.int32, (part, width), 1) // rank
    pair_level = jnp.minimum(lane_level, row_level)
    upper = pair_level >= low_levels
    below = lane_level < row_level
    equal = lane_level == row_level
    blank = jnp.zeros((part, low_width), f32)
    trees = []
    highs = []
    for half in range(2):
        rows_here = slice(half * part, (half + 1) * part)
        trees.append(node_sums([spread_ref[p, rows_here, :] for p in range(low_count)], low_levels))
        own, sibling = chain_sums(
            [high_ref[p, rows_here, :] for p in range(high_count)], place_ref[1], high_levels
        )
        picks = []
        for values in (own, sibling):
            pick = values[0]
            for level in range(1, high_levels):
                pick = jnp.where(
                    pair_level[:, low_width:] == low_levels + level, values[level], pick
                )
            picks.append(jnp.concatenate([blank, pick], axis=1))
        highs.append(picks)
    for p in range(low_count):
        own, sibling = [], []
        for half in range(2):
            mine, other = highs[half]
            for level in range(low_levels):
                chosen = pair_level == level
                mine = jnp.where(chosen, trees[half][level][p >> level], mine)
                other = jnp.where(chosen, trees[half][level][(p >> level) ^ 1], other)
            own.append(mine)
            sibling.append(other)
        ahead = own[0] + sibling[1]
        out_ref[p, :part, :] = jnp.where(
            below, sibling[0], jnp.where(equal, sibling[1], ahead)
        )
        out_ref[p, part:, :] = jnp.where(equal, sibling[0], sibling[1])


def operators_of(ref, rank):
    count, rows, width = ref.shape
    part = rows // 2
    first = ref[:, :part, :].reshape(count * part, width)
    second = ref[:, part:, :].reshape(count * part, width)
    row_level = lax.broadcasted_iota(jnp.int32, (width, width), 0) // rank
    lane_level = lax.broadcasted_iota(jnp.int32, (width, width), 1) // rank
    return first, second, lane_level > row_level


def eliminate_body(terms_ref, operators_ref, out_ref, *, rank):
    columns, width = terms_ref.shape
    count, share, _ = out_ref.shape
    first, _, ahead = operators_of(operators_ref, rank)
    feed = jnp.where(ahead, first, 0.0)
    half = width // 2

    def solve(value, square):
        double = full_dot(square, square)
        value = value - full_dot(value, square)
        return value + full_dot(value, double)

    early = solve(terms_ref[:, :half], feed[:half, :half])
    late = terms_ref[:, half:] - full_dot(early, feed[:half, half:])
    late = solve(late, feed[half:, half:])
    for j in range(count):
        rows = slice(j * share, (j + 1) * share)
        out_ref[j, :, :half] = early[rows, :]
        out_ref[j, :, half:] = late[rows, :]


def sums_body(place_ref, spread_ref, high_ref, out_ref, *, rank):
    low_count, share, width = spread_ref.shape
    high_count, _, high_width = high_ref.shape
    low_width = width - high_width
    low_levels = low_count.bit_length() - 1
    high_levels = high_count.bit_length() - 1
    lane_level = lax.broadcasted_iota(jnp.int32, (share, width), 1) // rank
    tree = node_sums([spread_ref[p] for p in range(low_count)], low_levels)
    blank = jnp.zeros((share, low_width), f32)
    highs = []
    for values in chain_sums([high_ref[p] for p in range(high_count)], place_ref[1], high_levels):
        pick = values[0]
        for level in range(1, high_levels):
            pick = jnp.where(lane_level[:, low_width:] == low_levels + level, values[level], pick)
        highs.append(jnp.concatenate([blank, pick], axis=1))
    for p in range(low_count):
        mine, other = highs
        for level in range(low_levels):
            chosen = lane_level == level
            mine = jnp.where(chosen, tree[level][p >> level], mine)
            other = jnp.where(chosen, tree[level][(p >> level) ^ 1], other)
        out_ref[p, :share, :] = mine
        out_ref[p, share:, :] = other


def weights_body(sums_ref, state_ref, basis_ref, coupling_ref, weights_ref, joined_ref, *, local_levels):
    count, rows, width = sums_ref.shape
    share = rows // 2
    columns = count * share
    rank = coupling_ref.shape[1]
    for j in range(count):
        joined_ref[j * share : (j + 1) * share, :] = sums_ref[j, :share, :]
        joined_ref[columns + j * share : columns + (j + 1) * share, :] = sums_ref[j, share:, :]
    pieces = []
    for level in range(width // rank):
        lanes = slice(level * rank, (level + 1) * rank)
        joined = jnp.concatenate(
            [joined_ref[:columns, lanes], joined_ref[columns:, lanes]], axis=1
        )
        pieces.append(full_dot(joined, coupling_ref[local_levels + level], rows_by_rows))
    mixed = jnp.concatenate(pieces, axis=1)
    update = wide_dot(mixed, basis_ref[local_levels * rank :, :], rows_by_columns)
    weights_ref[...] = (state_ref[...] - update).astype(bf16)


def mean_body(
    slots_ref, before_ref, mine_ref, after_ref, early_ref, late_ref, joined_ref, operators_ref,
    test_ref, out_ref, window_ref, near_ref, *, rank, leaf_size, factor,
):
    step = pl.program_id(0)
    steps = pl.num_programs(0)
    columns = mine_ref.shape[0]
    leaf_count = mine_ref.shape[1] // leaf_size

    @pl.when(step == 0)
    def _():
        for side, ref in enumerate((before_ref, mine_ref, after_ref)):
            for leaf in range(leaf_count):
                window_ref[side * leaf_count + leaf] = ref[
                    :, leaf * leaf_size : (leaf + 1) * leaf_size
                ]
        first, second, ahead = operators_of(operators_ref, rank)
        own = joined_ref[:columns, :]
        sibling = joined_ref[columns:, :]
        far = (
            sibling
            - full_dot(own, jnp.where(ahead, 0.0, first))
            - full_dot(sibling, jnp.where(ahead, 0.0, second))
        )
        near_ref[...] = wide_dot(far, test_ref[...], rows_by_columns) / factor

    near_ref[...] += jnp.dot(
        window_ref[slots_ref[step]], early_ref[0], preferred_element_type=f32
    ) + jnp.dot(window_ref[slots_ref[steps + step]], late_ref[0], preferred_element_type=f32)

    @pl.when(step == steps - 1)
    def _():
        out_ref[...] = (near_ref[...] * factor).astype(bf16)


def mean_kernel(slots, before, mine, after, early, late, joined, operators, test, rank, factor):
    steps, leaf_size, tests = early.shape
    columns, points = mine.shape
    whole = [before, mine, after]

    def fixed(array):
        return pl.BlockSpec(array.shape, lambda i, s: (0,) * array.ndim)

    moving = pl.BlockSpec((1, leaf_size, tests), lambda i, s: (i, 0, 0))

    def body(*refs):
        mean_body(*refs, rank=rank, leaf_size=leaf_size, factor=factor)

    return pl.pallas_call(
        body,
        out_shape=jax.ShapeDtypeStruct((columns, tests), bf16),
        grid_spec=pltpu.PrefetchScalarGridSpec(
            num_scalar_prefetch=1,
            grid=(steps,),
            in_specs=[fixed(a) for a in whole]
            + [moving, moving]
            + [fixed(a) for a in (joined, operators, test)],
            out_specs=pl.BlockSpec((columns, tests), lambda i, s: (0, 0)),
            scratch_shapes=[
                pltpu.VMEM((3 * points // leaf_size, columns, leaf_size), bf16),
                pltpu.VMEM((columns, tests), f32),
            ],
        ),
        name="posterior_mean",
    )(slots, *whole, early, late, joined, operators, test)


def exchange(value, axes):
    return lax.all_to_all(value, axes, 0, 0)


def gathered(value, axes):
    count = lax.axis_size(axes)
    return exchange(jnp.broadcast_to(value[None], (count,) + value.shape), axes)


def tie(*values):
    return lax.optimization_barrier(values)


def shards(
    targets,
    tree_order,
    leaf_inverse,
    cluster_basis,
    coupling,
    train_coords,
    test_coords,
    test_basis,
    near_leaves,
):
    columns, points = targets.shape
    leaf_count, leaf_size = leaf_inverse.shape[:2]
    all_levels, rank = cluster_basis.shape[:2]
    local_levels = leaf_count.bit_length() - 1
    low_count = lax.axis_size(low_axes)
    high_count = lax.axis_size("z")
    low_levels = low_count.bit_length() - 1
    low = lax.axis_index(low_axes)
    high = lax.axis_index("z")
    panels = low_count * high_count
    width = (all_levels - local_levels) * rank
    low_width = low_levels * rank
    part = width // low_count
    share = columns // low_count
    place = jnp.stack([low, high]).astype(jnp.int32)
    position = high * low_count + low
    basis = cluster_basis.reshape(all_levels * rank, points)
    mixers = coupling[0]
    half_slots = near_leaves.shape[1] // 2

    def mixer(*refs):
        mixer_body(*refs, local_levels=local_levels, part=part)

    effect = whole_call(
        mixer, jax.ShapeDtypeStruct((low_count, 2 * part, width), f32), "mixer"
    )(basis, mixers)
    spread = exchange(effect, low_axes)

    def featured(*refs):
        points_body(*refs, scale=3.0 / length_scale**2)

    features = jax.ShapeDtypeStruct((16, points), bf16)
    train_rows, test_rows = whole_call(
        featured, [features] * 2, "points", scratch=[pltpu.VMEM((16, points), f32)]
    )(train_coords, test_coords)
    forward = [(i, i + 1) for i in range(panels - 1)]
    backward = [(i + 1, i) for i in range(panels - 1)]
    sides = (
        lax.ppermute(train_rows, panel_axes, forward),
        train_rows,
        lax.ppermute(train_rows, panel_axes, backward),
    )

    state, terms = whole_call(
        local_body,
        [
            jax.ShapeDtypeStruct((columns, points), f32),
            jax.ShapeDtypeStruct((columns, width), f32),
        ],
        "local",
    )(targets, tree_order, leaf_inverse, basis, mixers)
    terms, spread = tie(terms, spread)

    window = jnp.concatenate(
        [rows.reshape(-1, leaf_count, leaf_size).transpose(1, 0, 2) for rows in sides], axis=0
    )
    slots = near_leaves[0] - (position - 1) * leaf_count
    total = jnp.sum(spread, axis=0)[:, low_width:]
    early_slots, total = tie(slots[:half_slots], total)
    high_spread = gathered(total, "z")
    early = distance_kernel(early_slots, window, test_rows, "near_early")
    early, high_spread = tie(early, high_spread)

    def operator(*refs):
        operator_body(*refs, rank=rank)

    operators = whole_call(
        operator, jax.ShapeDtypeStruct((low_count, 2 * part, width), f32), "operator", 1
    )(place, spread, high_spread)
    late_slots, operators = tie(slots[half_slots:], operators)
    operators = exchange(operators, low_axes)
    late = distance_kernel(late_slots, window, test_rows, "near_late")
    late, operators = tie(late, operators)

    def eliminate(*refs):
        eliminate_body(*refs, rank=rank)

    own_terms = whole_call(
        eliminate, jax.ShapeDtypeStruct((low_count, share, width), f32), "eliminate"
    )(terms, operators)
    spread = exchange(own_terms, low_axes)
    high_spread = gathered(jnp.sum(spread, axis=0)[:, low_width:], "z")

    def subtree(*refs):
        sums_body(*refs, rank=rank)

    sums = whole_call(
        subtree, jax.ShapeDtypeStruct((low_count, 2 * share, width), f32), "subtree", 1
    )(place, spread, high_spread)
    sums = exchange(sums, low_axes)

    def weigh(*refs):
        weights_body(*refs, local_levels=local_levels)

    weights, joined = whole_call(
        weigh,
        [
            jax.ShapeDtypeStruct((columns, points), bf16),
            jax.ShapeDtypeStruct((2 * columns, width), f32),
        ],
        "weights",
    )(sums, state, basis, mixers)
    before = lax.ppermute(weights, panel_axes, forward)
    after = lax.ppermute(weights, panel_axes, backward)
    return mean_kernel(
        slots,
        before,
        weights,
        after,
        early,
        late,
        joined,
        operators,
        test_basis.reshape(width, -1),
        rank,
        2.0 / math.sqrt(near_leaves.shape[1] * leaf_size),
    )


def solution(mesh):
    grp, leaf, sub = (mesh.shape[name] for name in ("grp", "leaf", "sub"))
    split = Mesh(mesh.devices.reshape(grp, leaf // 2, 2, sub), ("grp",) + panel_axes)
    every = ("grp",) + panel_axes
    return jax.shard_map(
        shards,
        mesh=split,
        in_specs=(
            P(None, every),
            P(every, None),
            P(every, None, None),
            P(None, None, every),
            P(every, None, None, None),
            P(None, every),
            P(None, every),
            P(None, None, every),
            P(every, None),
        ),
        out_specs=P(None, every),
        check_vma=False,
    )
```

```python
import math

import jax
import jax.numpy as jnp
from jax import lax
from jax.experimental import pallas as pl
from jax.experimental.pallas import tpu as pltpu
from jax.sharding import Mesh
from jax.sharding import PartitionSpec as P

length_scale = 0.5
highest = lax.Precision.HIGHEST
low_axes = ("core", "sub")
panel_axes = ("z", "core", "sub")
f32 = jnp.float32
bf16 = jnp.bfloat16
rows_by_columns = (((1,), (0,)), ((), ()))
rows_by_rows = (((1,), (1,)), ((), ()))
columns_by_columns = (((0,), (0,)), ((), ()))


def thirds(value):
    high = value.astype(bf16)
    rest = value - high.astype(f32)
    middle = rest.astype(bf16)
    low = (rest - middle.astype(f32)).astype(bf16)
    return high, middle, low


def wide_dot(left, right, dims):
    rows = left.shape[0]
    stacked = jnp.concatenate(thirds(left), axis=0)
    product = lax.dot_general(stacked, right, dims, preferred_element_type=f32)
    return product[:rows] + product[rows : 2 * rows] + product[2 * rows :]


def full_dot(left, right, dims=rows_by_columns):
    return lax.dot_general(left, right, dims, precision=highest, preferred_element_type=f32)


def whole_call(body, out_shape, name, scalars=0, scratch=()):
    def call(*operands):
        specs = [
            pl.BlockSpec(memory_space=pltpu.SMEM if i < scalars else pltpu.VMEM)
            for i in range(len(operands))
        ]
        single = not isinstance(out_shape, (list, tuple))
        out_specs = pl.BlockSpec(memory_space=pltpu.VMEM)
        return pl.pallas_call(
            body,
            out_shape=out_shape,
            in_specs=specs,
            out_specs=out_specs if single else [out_specs] * len(out_shape),
            scratch_shapes=list(scratch),
            name=name,
            compiler_params=pltpu.CompilerParams(vmem_limit_bytes=20 << 20),
        )(*operands)

    return call


def points_body(train_ref, test_ref, left_ref, right_ref, rows_ref, *, scale):
    dims, count = train_ref.shape
    ones = jnp.ones((1, count), f32)
    for ref, out_ref in ((train_ref, left_ref), (test_ref, right_ref)):
        exact = ref[...].astype(f32)
        norms = scale * jnp.sum(exact * exact, axis=0, keepdims=True)
        norms = [piece.astype(f32) for piece in thirds(norms)]
        if out_ref is left_ref:
            rows = [exact[axis : axis + 1] for axis in range(dims)] * 3 + norms + [ones] * 3
        else:
            pieces = [piece.astype(f32) for piece in thirds(-2.0 * scale * exact)]
            rows = [piece[axis : axis + 1] for piece in pieces for axis in range(dims)]
            rows = rows + [ones] * 3 + norms
        rows_ref[...] = jnp.zeros_like(rows_ref)
        for place, row in enumerate(rows):
            rows_ref[place : place + 1, :] = row
        out_ref[...] = rows_ref[...].astype(bf16)


def mixer_body(basis_ref, coupling_ref, out_ref, *, local_levels, part):
    rank = coupling_ref.shape[1]
    width = basis_ref.shape[0] - local_levels * rank
    points = basis_ref.shape[1]
    basis = basis_ref[local_levels * rank :, :]
    gram = lax.dot_general(basis, basis, rows_by_rows, preferred_element_type=f32)
    level = lax.broadcasted_iota(jnp.int32, (1, width), 1) // rank
    gram = gram * (lax.exp2(-0.5 * level.astype(f32)) / math.sqrt(points))
    for depth in range(width // rank):
        piece = gram[depth * rank : (depth + 1) * rank, :]
        product = full_dot(coupling_ref[local_levels + depth], piece, columns_by_columns)
        for half in range(2):
            for block in range(rank // part):
                start = half * rank + block * part
                out_ref[depth * (rank // part) + block, half * part : (half + 1) * part, :] = (
                    product[start : start + part, :]
                )


def local_body(targets_ref, order_ref, inverse_ref, basis_ref, coupling_ref, state_ref, terms_ref):
    columns, points = targets_ref.shape
    leaf_count, leaf_size, _ = inverse_ref.shape
    rank = coupling_ref.shape[1]
    local_levels = leaf_count.bit_length() - 1
    place = lax.broadcasted_iota(jnp.int32, (points, leaf_size), 0)
    for leaf in range(leaf_count):
        lanes = slice(leaf * leaf_size, (leaf + 1) * leaf_size)
        chosen = jnp.where(place == order_ref[:, lanes], 1.0, 0.0).astype(bf16)
        block = jnp.dot(targets_ref[...], chosen, preferred_element_type=f32).astype(bf16)
        state_ref[:, lanes] = lax.dot_general(
            block, inverse_ref[leaf], rows_by_rows, preferred_element_type=f32
        )
    for level in range(local_levels):
        child = leaf_size << level
        count = points // child
        mixers = coupling_ref[level]
        bases = [
            basis_ref[level * rank : (level + 1) * rank, c * child : (c + 1) * child]
            for c in range(count)
        ]
        sums = [
            wide_dot(state_ref[:, c * child : (c + 1) * child], bases[c], rows_by_rows)
            / math.sqrt(child)
            for c in range(count)
        ]
        for c in range(count):
            joined = jnp.concatenate([sums[c], sums[c ^ 1]], axis=1)
            mixed = full_dot(joined, mixers, rows_by_rows)
            lanes = slice(c * child, (c + 1) * child)
            state_ref[:, lanes] = state_ref[:, lanes] - wide_dot(mixed, bases[c], rows_by_columns)
    width = terms_ref.shape[1]
    level = lax.broadcasted_iota(jnp.int32, (1, width), 1) // rank
    scale = lax.exp2(-0.5 * level.astype(f32)) / math.sqrt(points)
    terms_ref[...] = (
        wide_dot(state_ref[...], basis_ref[local_levels * rank :, :], rows_by_rows) * scale
    )


def distance_body(slots_ref, before_ref, mine_ref, after_ref, test_ref, out_ref, train_ref):
    leaf = slots_ref[pl.program_id(0)]
    leaf_size = train_ref.shape[1]
    leaf_count = mine_ref.shape[1] // leaf_size
    for side, ref in enumerate((before_ref, mine_ref, after_ref)):

        @pl.when(leaf // leaf_count == side)
        def _(ref=ref):
            start = pl.multiple_of((leaf % leaf_count) * leaf_size, leaf_size)
            train_ref[...] = ref[:, pl.ds(start, leaf_size)]

    train = train_ref[...]
    step = 256
    for start in range(0, test_ref.shape[1], step):
        squared = lax.dot_general(
            train, test_ref[:, start : start + step], columns_by_columns,
            preferred_element_type=f32,
        )
        squared = jnp.maximum(squared, 1e-20)
        scaled = squared * lax.rsqrt(squared)
        out_ref[0, :, start : start + step] = ((1.0 + scaled) * jnp.exp(-scaled)).astype(bf16)


def distance_kernel(slots, sides, test_features, leaf_size, name):
    tests = test_features.shape[1]
    operands = (*sides, test_features)
    return pl.pallas_call(
        distance_body,
        out_shape=pltpu.HBM((slots.shape[0], leaf_size, tests), bf16),
        grid_spec=pltpu.PrefetchScalarGridSpec(
            num_scalar_prefetch=1,
            grid=(slots.shape[0],),
            in_specs=[pl.BlockSpec(a.shape, lambda i, s: (0, 0)) for a in operands],
            out_specs=pl.BlockSpec((1, leaf_size, tests), lambda i, s: (i, 0, 0)),
            scratch_shapes=[pltpu.VMEM((sides[0].shape[0], leaf_size), bf16)],
        ),
        compiler_params=pltpu.CompilerParams(vmem_limit_bytes=24 << 20),
        name=name,
    )(slots, *operands)


def node_sums(members, levels):
    sums = [members]
    for _ in range(levels):
        last = sums[-1]
        sums.append([last[i] + last[i + 1] for i in range(0, len(last), 2)])
    return sums


def chain_sums(values, position, levels):
    tree = node_sums(values, levels)
    own, sibling = [], []
    for level in range(levels):
        nodes = tree[level]
        mine = position >> level
        first, second = nodes[0], nodes[1]
        for node in range(2, len(nodes), 2):
            here = (mine >> 1) == (node >> 1)
            first = jnp.where(here, nodes[node], first)
            second = jnp.where(here, nodes[node + 1], second)
        right = (mine & 1) == 1
        own.append(jnp.where(right, second, first))
        sibling.append(jnp.where(right, first, second))
    return own, sibling


def operator_body(place_ref, spread_ref, high_ref, out_ref, *, rank):
    low_count, rows, width = spread_ref.shape
    part = rows // 2
    high_count, _, high_width = high_ref.shape
    low_width = width - high_width
    low_levels = low_count.bit_length() - 1
    high_levels = high_count.bit_length() - 1
    row_level = place_ref[0] * part // rank
    lane_level = lax.broadcasted_iota(jnp.int32, (part, width), 1) // rank
    pair_level = jnp.minimum(lane_level, row_level)
    upper = pair_level >= low_levels
    below = lane_level < row_level
    equal = lane_level == row_level
    blank = jnp.zeros((part, low_width), f32)
    trees = []
    highs = []
    for half in range(2):
        rows_here = slice(half * part, (half + 1) * part)
        trees.append(node_sums([spread_ref[p, rows_here, :] for p in range(low_count)], low_levels))
        own, sibling = chain_sums(
            [high_ref[p, rows_here, :] for p in range(high_count)], place_ref[1], high_levels
        )
        picks = []
        for values in (own, sibling):
            pick = values[0]
            for level in range(1, high_levels):
                pick = jnp.where(
                    pair_level[:, low_width:] == low_levels + level, values[level], pick
                )
            picks.append(jnp.concatenate([blank, pick], axis=1))
        highs.append(picks)
    for p in range(low_count):
        own, sibling = [], []
        for half in range(2):
            mine, other = highs[half]
            for level in range(low_levels):
                chosen = pair_level == level
                mine = jnp.where(chosen, trees[half][level][p >> level], mine)
                other = jnp.where(chosen, trees[half][level][(p >> level) ^ 1], other)
            own.append(mine)
            sibling.append(other)
        ahead = own[0] + sibling[1]
        first = jnp.where(below, sibling[0], jnp.where(equal, sibling[1], ahead))
        high = first.astype(bf16)
        out_ref[p, :part, :] = high
        out_ref[p, part : 2 * part, :] = (first - high.astype(f32)).astype(bf16)
        out_ref[p, 2 * part :, :] = jnp.where(equal, sibling[0], sibling[1]).astype(bf16)


def operators_of(ref, rank):
    count, rows, width = ref.shape
    part = rows // 3
    first, rest, second = (
        ref[:, i * part : (i + 1) * part, :].reshape(count * part, width).astype(f32)
        for i in range(3)
    )
    first = first + rest
    row_level = lax.broadcasted_iota(jnp.int32, (width, width), 0) // rank
    lane_level = lax.broadcasted_iota(jnp.int32, (width, width), 1) // rank
    return first, second, lane_level > row_level


def eliminate_body(terms_ref, operators_ref, out_ref, *, rank):
    columns, width = terms_ref.shape
    count, share, _ = out_ref.shape
    first, _, ahead = operators_of(operators_ref, rank)
    feed = jnp.where(ahead, first, 0.0)
    half = width // 2

    def solve(value, square):
        double = full_dot(square, square)
        value = value - full_dot(value, square)
        return value + full_dot(value, double)

    early = solve(terms_ref[:, :half], feed[:half, :half])
    late = terms_ref[:, half:] - full_dot(early, feed[:half, half:])
    late = solve(late, feed[half:, half:])
    for j in range(count):
        rows = slice(j * share, (j + 1) * share)
        out_ref[j, :, :half] = early[rows, :]
        out_ref[j, :, half:] = late[rows, :]


def sums_body(place_ref, spread_ref, high_ref, out_ref, *, rank):
    low_count, share, width = spread_ref.shape
    high_count, _, high_width = high_ref.shape
    low_width = width - high_width
    low_levels = low_count.bit_length() - 1
    high_levels = high_count.bit_length() - 1
    lane_level = lax.broadcasted_iota(jnp.int32, (share, width), 1) // rank
    tree = node_sums([spread_ref[p] for p in range(low_count)], low_levels)
    blank = jnp.zeros((share, low_width), f32)
    highs = []
    for values in chain_sums([high_ref[p] for p in range(high_count)], place_ref[1], high_levels):
        pick = values[0]
        for level in range(1, high_levels):
            pick = jnp.where(lane_level[:, low_width:] == low_levels + level, values[level], pick)
        highs.append(jnp.concatenate([blank, pick], axis=1))
    for p in range(low_count):
        mine, other = highs
        for level in range(low_levels):
            chosen = lane_level == level
            mine = jnp.where(chosen, tree[level][p >> level], mine)
            other = jnp.where(chosen, tree[level][(p >> level) ^ 1], other)
        out_ref[p, :share, :] = mine
        out_ref[p, share:, :] = other


def weights_body(sums_ref, state_ref, basis_ref, coupling_ref, weights_ref, joined_ref, *, local_levels):
    count, rows, width = sums_ref.shape
    share = rows // 2
    columns = count * share
    rank = coupling_ref.shape[1]
    for j in range(count):
        joined_ref[j * share : (j + 1) * share, :] = sums_ref[j, :share, :]
        joined_ref[columns + j * share : columns + (j + 1) * share, :] = sums_ref[j, share:, :]
    pieces = []
    for level in range(width // rank):
        lanes = slice(level * rank, (level + 1) * rank)
        joined = jnp.concatenate(
            [joined_ref[:columns, lanes], joined_ref[columns:, lanes]], axis=1
        )
        pieces.append(full_dot(joined, coupling_ref[local_levels + level], rows_by_rows))
    mixed = jnp.concatenate(pieces, axis=1)
    update = wide_dot(mixed, basis_ref[local_levels * rank :, :], rows_by_columns)
    weights_ref[...] = (state_ref[...] - update).astype(bf16)


def far_body(joined_ref, operators_ref, test_ref, out_ref, *, rank, factor):
    columns = out_ref.shape[0]
    first, second, ahead = operators_of(operators_ref, rank)
    own = joined_ref[:columns, :]
    sibling = joined_ref[columns:, :]
    far = (
        sibling
        - full_dot(own, jnp.where(ahead, 0.0, first))
        - full_dot(sibling, jnp.where(ahead, 0.0, second))
    )
    out_ref[...] = wide_dot(far, test_ref[...], rows_by_columns) / factor


def mean_body(
    slots_ref, before_ref, mine_ref, after_ref, early_ref, late_ref, far_ref,
    out_ref, window_ref, near_ref, *, leaf_size, factor,
):
    step = pl.program_id(0)
    steps = pl.num_programs(0)
    columns = mine_ref.shape[0]
    leaf_count = mine_ref.shape[1] // leaf_size

    @pl.when(step == 0)
    def _():
        for side, ref in enumerate((before_ref, mine_ref, after_ref)):
            for leaf in range(leaf_count):
                window_ref[side * leaf_count + leaf] = ref[
                    :, leaf * leaf_size : (leaf + 1) * leaf_size
                ]
        near_ref[...] = far_ref[...]

    near_ref[...] += jnp.dot(
        window_ref[slots_ref[step]], early_ref[0], preferred_element_type=f32
    ) + jnp.dot(window_ref[slots_ref[steps + step]], late_ref[0], preferred_element_type=f32)

    @pl.when(step == steps - 1)
    def _():
        out_ref[...] = (near_ref[...] * factor).astype(bf16)


def in_hbm(value):
    return pltpu.with_memory_space_constraint(value, pltpu.HBM)


def mean_kernel(slots, before, mine, after, early, late, far, factor):
    steps, leaf_size, tests = early.shape
    columns, points = mine.shape
    whole = [before, mine, after]

    def fixed(array):
        return pl.BlockSpec(array.shape, lambda i, s: (0,) * array.ndim)

    moving = pl.BlockSpec((1, leaf_size, tests), lambda i, s: (i, 0, 0))

    def body(*refs):
        mean_body(*refs, leaf_size=leaf_size, factor=factor)

    return pl.pallas_call(
        body,
        out_shape=jax.ShapeDtypeStruct((columns, tests), bf16),
        grid_spec=pltpu.PrefetchScalarGridSpec(
            num_scalar_prefetch=1,
            grid=(steps,),
            in_specs=[fixed(a) for a in whole]
            + [moving, moving]
            + [fixed(far)],
            out_specs=pl.BlockSpec((columns, tests), lambda i, s: (0, 0)),
            scratch_shapes=[
                pltpu.VMEM((3 * points // leaf_size, columns, leaf_size), bf16),
                pltpu.VMEM((columns, tests), f32),
            ],
        ),
        compiler_params=pltpu.CompilerParams(vmem_limit_bytes=24 << 20),
        name="posterior_mean",
    )(slots, *whole, in_hbm(early), in_hbm(late), far)


def exchange(value, axes):
    return lax.all_to_all(value, axes, 0, 0)


def gathered(value, axes):
    count = lax.axis_size(axes)
    return exchange(jnp.broadcast_to(value[None], (count,) + value.shape), axes)


def tie(*values):
    return lax.optimization_barrier(values)


def shards(
    targets,
    tree_order,
    leaf_inverse,
    cluster_basis,
    coupling,
    train_coords,
    test_coords,
    test_basis,
    near_leaves,
):
    columns, points = targets.shape
    leaf_count, leaf_size = leaf_inverse.shape[:2]
    all_levels, rank = cluster_basis.shape[:2]
    local_levels = leaf_count.bit_length() - 1
    low_count = lax.axis_size(low_axes)
    high_count = lax.axis_size("z")
    low_levels = low_count.bit_length() - 1
    low = lax.axis_index(low_axes)
    high = lax.axis_index("z")
    panels = low_count * high_count
    width = (all_levels - local_levels) * rank
    low_width = low_levels * rank
    part = width // low_count
    share = columns // low_count
    place = jnp.stack([low, high]).astype(jnp.int32)
    position = high * low_count + low
    basis = cluster_basis.reshape(all_levels * rank, points)
    mixers = coupling[0]
    half_slots = near_leaves.shape[1] // 2

    def mixer(*refs):
        mixer_body(*refs, local_levels=local_levels, part=part)

    effect = whole_call(
        mixer, jax.ShapeDtypeStruct((low_count, 2 * part, width), f32), "mixer"
    )(basis, mixers)
    effect, train_coords = tie(effect, train_coords)
    spread = exchange(effect, low_axes)

    def featured(*refs):
        points_body(*refs, scale=3.0 / length_scale**2)

    features = jax.ShapeDtypeStruct((16, points), bf16)
    train_rows, test_rows = whole_call(
        featured, [features] * 2, "points", scratch=[pltpu.VMEM((16, points), f32)]
    )(train_coords, test_coords)
    forward = [(i, i + 1) for i in range(panels - 1)]
    backward = [(i + 1, i) for i in range(panels - 1)]
    sides = (
        lax.ppermute(train_rows, panel_axes, forward),
        train_rows,
        lax.ppermute(train_rows, panel_axes, backward),
    )
    *sides, tree_order = tie(*sides, tree_order)

    state, terms = whole_call(
        local_body,
        [
            jax.ShapeDtypeStruct((columns, points), f32),
            jax.ShapeDtypeStruct((columns, width), f32),
        ],
        "local",
    )(targets, tree_order, leaf_inverse, basis, mixers)
    terms, spread = tie(terms, spread)

    slots = near_leaves[0] - (position - 1) * leaf_count
    total = jnp.sum(spread, axis=0)[:, low_width:]
    early_slots, total = tie(slots[:half_slots], total)
    high_spread = gathered(total, "z")
    early = distance_kernel(early_slots, sides, test_rows, leaf_size, "near_early")
    early, high_spread = tie(early, high_spread)

    def operator(*refs):
        operator_body(*refs, rank=rank)

    operators = whole_call(
        operator, jax.ShapeDtypeStruct((low_count, 3 * part, width), bf16), "operator", 1
    )(place, spread, high_spread)
    late_slots, operators = tie(slots[half_slots:], operators)
    operators = exchange(operators, low_axes)
    late = distance_kernel(late_slots, sides, test_rows, leaf_size, "near_late")
    late, operators = tie(late, operators)

    def eliminate(*refs):
        eliminate_body(*refs, rank=rank)

    own_terms = whole_call(
        eliminate, jax.ShapeDtypeStruct((low_count, share, width), f32), "eliminate"
    )(terms, operators)
    spread = exchange(own_terms, low_axes)
    high_spread = gathered(jnp.sum(spread, axis=0)[:, low_width:], "z")

    def subtree(*refs):
        sums_body(*refs, rank=rank)

    sums = whole_call(
        subtree, jax.ShapeDtypeStruct((low_count, 2 * share, width), f32), "subtree", 1
    )(place, spread, high_spread)
    sums = exchange(sums, low_axes)

    def weigh(*refs):
        weights_body(*refs, local_levels=local_levels)

    weights, joined = whole_call(
        weigh,
        [
            jax.ShapeDtypeStruct((columns, points), bf16),
            jax.ShapeDtypeStruct((2 * columns, width), f32),
        ],
        "weights",
    )(sums, state, basis, mixers)
    before = lax.ppermute(weights, panel_axes, forward)
    after = lax.ppermute(weights, panel_axes, backward)
    factor = 2.0 / math.sqrt(near_leaves.shape[1] * leaf_size)

    def distant(*refs):
        far_body(*refs, rank=rank, factor=factor)

    far = whole_call(distant, jax.ShapeDtypeStruct((columns, points), f32), "far")(
        joined, operators, test_basis.reshape(width, -1)
    )
    return mean_kernel(slots, before, weights, after, early, late, far, factor)


def solution(mesh):
    grp, leaf, sub = (mesh.shape[name] for name in ("grp", "leaf", "sub"))
    split = Mesh(mesh.devices.reshape(grp, leaf // 2, 2, sub), ("grp",) + panel_axes)
    every = ("grp",) + panel_axes
    return jax.shard_map(
        shards,
        mesh=split,
        in_specs=(
            P(None, every),
            P(every, None),
            P(every, None, None),
            P(None, None, every),
            P(every, None, None, None),
            P(None, every),
            P(None, every),
            P(None, None, every),
            P(every, None),
        ),
        out_specs=P(None, every),
        check_vma=False,
    )
```

```python
import math

import jax
import jax.numpy as jnp
from jax import lax
from jax.experimental import pallas as pl
from jax.experimental.pallas import tpu as pltpu
from jax.sharding import Mesh
from jax.sharding import PartitionSpec as P

length_scale = 0.5
highest = lax.Precision.HIGHEST
low_axes = ("core", "sub")
panel_axes = ("z", "core", "sub")
f32 = jnp.float32
bf16 = jnp.bfloat16
rows_by_columns = (((1,), (0,)), ((), ()))
rows_by_rows = (((1,), (1,)), ((), ()))
columns_by_columns = (((0,), (0,)), ((), ()))


def thirds(value):
    high = value.astype(bf16)
    rest = value - high.astype(f32)
    middle = rest.astype(bf16)
    low = (rest - middle.astype(f32)).astype(bf16)
    return high, middle, low


def wide_dot(left, right, dims):
    rows = left.shape[0]
    stacked = jnp.concatenate(thirds(left), axis=0)
    product = lax.dot_general(stacked, right, dims, preferred_element_type=f32)
    return product[:rows] + product[rows : 2 * rows] + product[2 * rows :]


def full_dot(left, right, dims=rows_by_columns):
    return lax.dot_general(left, right, dims, precision=highest, preferred_element_type=f32)


def whole_call(body, out_shape, name, scalars=0, scratch=(), limit=20 << 20):
    def call(*operands):
        specs = [
            pl.BlockSpec(memory_space=pltpu.SMEM if i < scalars else pltpu.VMEM)
            for i in range(len(operands))
        ]
        single = not isinstance(out_shape, (list, tuple))
        out_specs = pl.BlockSpec(memory_space=pltpu.VMEM)
        return pl.pallas_call(
            body,
            out_shape=out_shape,
            in_specs=specs,
            out_specs=out_specs if single else [out_specs] * len(out_shape),
            scratch_shapes=list(scratch),
            name=name,
            compiler_params=pltpu.CompilerParams(vmem_limit_bytes=limit),
        )(*operands)

    return call


def points_body(train_ref, test_ref, left_ref, right_ref, rows_ref, *, scale):
    dims, count = train_ref.shape
    ones = jnp.ones((1, count), f32)
    for ref, out_ref in ((train_ref, left_ref), (test_ref, right_ref)):
        exact = ref[...].astype(f32)
        norms = scale * jnp.sum(exact * exact, axis=0, keepdims=True)
        norms = [piece.astype(f32) for piece in thirds(norms)]
        if out_ref is left_ref:
            rows = [exact[axis : axis + 1] for axis in range(dims)] * 3 + norms + [ones] * 3
        else:
            pieces = [piece.astype(f32) for piece in thirds(-2.0 * scale * exact)]
            rows = [piece[axis : axis + 1] for piece in pieces for axis in range(dims)]
            rows = rows + [ones] * 3 + norms
        rows_ref[...] = jnp.zeros_like(rows_ref)
        for place, row in enumerate(rows):
            rows_ref[place : place + 1, :] = row
        out_ref[...] = rows_ref[...].astype(bf16)


def mixer_body(basis_ref, coupling_ref, out_ref, *, local_levels, part):
    rank = coupling_ref.shape[1]
    width = basis_ref.shape[0] - local_levels * rank
    points = basis_ref.shape[1]
    basis = basis_ref[local_levels * rank :, :]
    gram = lax.dot_general(basis, basis, rows_by_rows, preferred_element_type=f32)
    level = lax.broadcasted_iota(jnp.int32, (1, width), 1) // rank
    gram = gram * (lax.exp2(-0.5 * level.astype(f32)) / math.sqrt(points))
    for depth in range(width // rank):
        piece = gram[depth * rank : (depth + 1) * rank, :]
        product = full_dot(coupling_ref[local_levels + depth], piece, columns_by_columns)
        for half in range(2):
            for block in range(rank // part):
                start = half * rank + block * part
                out_ref[depth * (rank // part) + block, half * part : (half + 1) * part, :] = (
                    product[start : start + part, :]
                )


def local_body(targets_ref, order_ref, inverse_ref, basis_ref, coupling_ref, state_ref, terms_ref):
    columns, points = targets_ref.shape
    leaf_count, leaf_size, _ = inverse_ref.shape
    rank = coupling_ref.shape[1]
    local_levels = leaf_count.bit_length() - 1
    place = lax.broadcasted_iota(jnp.int32, (points, leaf_size), 0)
    for leaf in range(leaf_count):
        lanes = slice(leaf * leaf_size, (leaf + 1) * leaf_size)
        chosen = jnp.where(place == order_ref[:, lanes], 1.0, 0.0).astype(bf16)
        block = jnp.dot(targets_ref[...], chosen, preferred_element_type=f32).astype(bf16)
        state_ref[:, lanes] = lax.dot_general(
            block, inverse_ref[leaf], rows_by_rows, preferred_element_type=f32
        )
    for level in range(local_levels):
        child = leaf_size << level
        count = points // child
        mixers = coupling_ref[level]
        bases = [
            basis_ref[level * rank : (level + 1) * rank, c * child : (c + 1) * child]
            for c in range(count)
        ]
        sums = [
            wide_dot(state_ref[:, c * child : (c + 1) * child], bases[c], rows_by_rows)
            / math.sqrt(child)
            for c in range(count)
        ]
        for c in range(count):
            joined = jnp.concatenate([sums[c], sums[c ^ 1]], axis=1)
            mixed = full_dot(joined, mixers, rows_by_rows)
            lanes = slice(c * child, (c + 1) * child)
            state_ref[:, lanes] = state_ref[:, lanes] - wide_dot(mixed, bases[c], rows_by_columns)
    width = terms_ref.shape[1]
    level = lax.broadcasted_iota(jnp.int32, (1, width), 1) // rank
    scale = lax.exp2(-0.5 * level.astype(f32)) / math.sqrt(points)
    terms_ref[...] = (
        wide_dot(state_ref[...], basis_ref[local_levels * rank :, :], rows_by_rows) * scale
    )


def distance_body(slots_ref, before_ref, mine_ref, after_ref, test_ref, out_ref, train_ref):
    leaf = slots_ref[pl.program_id(0)]
    leaf_size = train_ref.shape[1]
    leaf_count = mine_ref.shape[1] // leaf_size
    for side, ref in enumerate((before_ref, mine_ref, after_ref)):

        @pl.when(leaf // leaf_count == side)
        def _(ref=ref):
            start = pl.multiple_of((leaf % leaf_count) * leaf_size, leaf_size)
            train_ref[...] = ref[:, pl.ds(start, leaf_size)]

    train = train_ref[...]
    step = 256
    for start in range(0, test_ref.shape[1], step):
        squared = lax.dot_general(
            train, test_ref[:, start : start + step], columns_by_columns,
            preferred_element_type=f32,
        )
        squared = jnp.maximum(squared, 1e-20)
        scaled = squared * lax.rsqrt(squared)
        out_ref[0, :, start : start + step] = ((1.0 + scaled) * jnp.exp(-scaled)).astype(bf16)


def distance_kernel(slots, sides, test_features, leaf_size, name, store=pltpu.HBM):
    tests = test_features.shape[1]
    operands = (*sides, test_features)
    return pl.pallas_call(
        distance_body,
        out_shape=store((slots.shape[0], leaf_size, tests), bf16),
        grid_spec=pltpu.PrefetchScalarGridSpec(
            num_scalar_prefetch=1,
            grid=(slots.shape[0],),
            in_specs=[pl.BlockSpec(a.shape, lambda i, s: (0, 0)) for a in operands],
            out_specs=pl.BlockSpec((1, leaf_size, tests), lambda i, s: (i, 0, 0)),
            scratch_shapes=[pltpu.VMEM((sides[0].shape[0], leaf_size), bf16)],
        ),
        compiler_params=pltpu.CompilerParams(vmem_limit_bytes=24 << 20),
        name=name,
    )(slots, *operands)


def node_sums(members, levels):
    sums = [members]
    for _ in range(levels):
        last = sums[-1]
        sums.append([last[i] + last[i + 1] for i in range(0, len(last), 2)])
    return sums


def chain_sums(values, position, levels):
    tree = node_sums(values, levels)
    own, sibling = [], []
    for level in range(levels):
        nodes = tree[level]
        mine = position >> level
        first, second = nodes[0], nodes[1]
        for node in range(2, len(nodes), 2):
            here = (mine >> 1) == (node >> 1)
            first = jnp.where(here, nodes[node], first)
            second = jnp.where(here, nodes[node + 1], second)
        right = (mine & 1) == 1
        own.append(jnp.where(right, second, first))
        sibling.append(jnp.where(right, first, second))
    return own, sibling


def operator_body(place_ref, spread_ref, high_ref, out_ref, *, rank):
    low_count, rows, width = spread_ref.shape
    part = rows // 2
    high_count, _, high_width = high_ref.shape
    low_width = width - high_width
    low_levels = low_count.bit_length() - 1
    high_levels = high_count.bit_length() - 1
    row_level = place_ref[0] * part // rank
    lane_level = lax.broadcasted_iota(jnp.int32, (part, width), 1) // rank
    pair_level = jnp.minimum(lane_level, row_level)
    upper = pair_level >= low_levels
    below = lane_level < row_level
    equal = lane_level == row_level
    blank = jnp.zeros((part, low_width), f32)
    trees = []
    highs = []
    for half in range(2):
        rows_here = slice(half * part, (half + 1) * part)
        trees.append(node_sums([spread_ref[p, rows_here, :] for p in range(low_count)], low_levels))
        own, sibling = chain_sums(
            [high_ref[p, rows_here, :] for p in range(high_count)], place_ref[1], high_levels
        )
        picks = []
        for values in (own, sibling):
            pick = values[0]
            for level in range(1, high_levels):
                pick = jnp.where(
                    pair_level[:, low_width:] == low_levels + level, values[level], pick
                )
            picks.append(jnp.concatenate([blank, pick], axis=1))
        highs.append(picks)
    for p in range(low_count):
        own, sibling = [], []
        for half in range(2):
            mine, other = highs[half]
            for level in range(low_levels):
                chosen = pair_level == level
                mine = jnp.where(chosen, trees[half][level][p >> level], mine)
                other = jnp.where(chosen, trees[half][level][(p >> level) ^ 1], other)
            own.append(mine)
            sibling.append(other)
        ahead = own[0] + sibling[1]
        first = jnp.where(below, sibling[0], jnp.where(equal, sibling[1], ahead))
        high = first.astype(bf16)
        out_ref[p, :part, :] = high
        out_ref[p, part : 2 * part, :] = (first - high.astype(f32)).astype(bf16)
        out_ref[p, 2 * part :, :] = jnp.where(equal, sibling[0], sibling[1]).astype(bf16)


def operators_of(ref, rank):
    count, rows, width = ref.shape
    part = rows // 3
    first, rest, second = (
        ref[:, i * part : (i + 1) * part, :].reshape(count * part, width).astype(f32)
        for i in range(3)
    )
    first = first + rest
    row_level = lax.broadcasted_iota(jnp.int32, (width, width), 0) // rank
    lane_level = lax.broadcasted_iota(jnp.int32, (width, width), 1) // rank
    return first, second, lane_level > row_level


def eliminate_body(terms_ref, operators_ref, out_ref, *, rank):
    columns, width = terms_ref.shape
    count, share, _ = out_ref.shape
    first, _, ahead = operators_of(operators_ref, rank)
    feed = jnp.where(ahead, first, 0.0)
    half = width // 2

    def solve(value, square):
        double = full_dot(square, square)
        value = value - full_dot(value, square)
        return value + full_dot(value, double)

    early = solve(terms_ref[:, :half], feed[:half, :half])
    late = terms_ref[:, half:] - full_dot(early, feed[:half, half:])
    late = solve(late, feed[half:, half:])
    for j in range(count):
        rows = slice(j * share, (j + 1) * share)
        out_ref[j, :, :half] = early[rows, :]
        out_ref[j, :, half:] = late[rows, :]


def sums_body(place_ref, spread_ref, high_ref, out_ref, *, rank):
    low_count, share, width = spread_ref.shape
    high_count, _, high_width = high_ref.shape
    low_width = width - high_width
    low_levels = low_count.bit_length() - 1
    high_levels = high_count.bit_length() - 1
    lane_level = lax.broadcasted_iota(jnp.int32, (share, width), 1) // rank
    tree = node_sums([spread_ref[p] for p in range(low_count)], low_levels)
    blank = jnp.zeros((share, low_width), f32)
    highs = []
    for values in chain_sums([high_ref[p] for p in range(high_count)], place_ref[1], high_levels):
        pick = values[0]
        for level in range(1, high_levels):
            pick = jnp.where(lane_level[:, low_width:] == low_levels + level, values[level], pick)
        highs.append(jnp.concatenate([blank, pick], axis=1))
    for p in range(low_count):
        mine, other = highs
        for level in range(low_levels):
            chosen = lane_level == level
            mine = jnp.where(chosen, tree[level][p >> level], mine)
            other = jnp.where(chosen, tree[level][(p >> level) ^ 1], other)
        out_ref[p, :share, :] = mine
        out_ref[p, share:, :] = other


def weights_body(sums_ref, state_ref, basis_ref, coupling_ref, weights_ref, joined_ref, *, local_levels):
    count, rows, width = sums_ref.shape
    share = rows // 2
    columns = count * share
    rank = coupling_ref.shape[1]
    for j in range(count):
        joined_ref[j * share : (j + 1) * share, :] = sums_ref[j, :share, :]
        joined_ref[columns + j * share : columns + (j + 1) * share, :] = sums_ref[j, share:, :]
    pieces = []
    for level in range(width // rank):
        lanes = slice(level * rank, (level + 1) * rank)
        joined = jnp.concatenate(
            [joined_ref[:columns, lanes], joined_ref[columns:, lanes]], axis=1
        )
        pieces.append(full_dot(joined, coupling_ref[local_levels + level], rows_by_rows))
    mixed = jnp.concatenate(pieces, axis=1)
    update = wide_dot(mixed, basis_ref[local_levels * rank :, :], rows_by_columns)
    weights_ref[...] = (state_ref[...] - update).astype(bf16)


def far_body(joined_ref, operators_ref, test_ref, out_ref, *, rank, factor):
    columns = out_ref.shape[0]
    first, second, ahead = operators_of(operators_ref, rank)
    own = joined_ref[:columns, :]
    sibling = joined_ref[columns:, :]
    far = (
        sibling
        - full_dot(own, jnp.where(ahead, 0.0, first))
        - full_dot(sibling, jnp.where(ahead, 0.0, second))
    )
    out_ref[...] = wide_dot(far, test_ref[...], rows_by_columns) / factor


def mean_body(
    slots_ref, before_ref, mine_ref, after_ref, early_ref, late_ref, last_ref, far_ref,
    out_ref, window_ref, near_ref, *, leaf_size, factor,
):
    step = pl.program_id(0)
    steps = pl.num_programs(0)
    columns = mine_ref.shape[0]
    leaf_count = mine_ref.shape[1] // leaf_size

    @pl.when(step == 0)
    def _():
        for side, ref in enumerate((before_ref, mine_ref, after_ref)):
            for leaf in range(leaf_count):
                window_ref[side * leaf_count + leaf] = ref[
                    :, leaf * leaf_size : (leaf + 1) * leaf_size
                ]
        near_ref[...] = far_ref[...]

    def part_of(slot, ref):
        return jnp.dot(window_ref[slots_ref[slot]], ref[0], preferred_element_type=f32)

    @pl.when(step < steps - 1)
    def _():
        near_ref[...] += part_of(step, early_ref) + part_of(steps + step, late_ref)

    @pl.when(step == steps - 1)
    def _():
        near = near_ref[...] + part_of(step, early_ref) + part_of(steps + step, last_ref)
        out_ref[...] = (near * factor).astype(bf16)


def in_hbm(value):
    return pltpu.with_memory_space_constraint(value, pltpu.HBM)


def mean_kernel(slots, before, mine, after, early, late, last, far, factor):
    steps, leaf_size, tests = early.shape
    columns, points = mine.shape
    whole = [before, mine, after]

    def fixed(array):
        return pl.BlockSpec(array.shape, lambda i, s: (0,) * array.ndim)

    block = (1, leaf_size, tests)
    final = late.shape[0] - 1
    moving = [
        pl.BlockSpec(block, lambda i, s: (i, 0, 0)),
        pl.BlockSpec(block, lambda i, s: (jnp.minimum(i, final), 0, 0)),
        pl.BlockSpec(memory_space=pltpu.VMEM),
    ]

    def body(*refs):
        mean_body(*refs, leaf_size=leaf_size, factor=factor)

    return pl.pallas_call(
        body,
        out_shape=jax.ShapeDtypeStruct((columns, tests), bf16),
        grid_spec=pltpu.PrefetchScalarGridSpec(
            num_scalar_prefetch=1,
            grid=(steps,),
            in_specs=[fixed(a) for a in whole]
            + moving
            + [fixed(far)],
            out_specs=pl.BlockSpec((columns, tests), lambda i, s: (0, 0)),
            scratch_shapes=[
                pltpu.VMEM((3 * points // leaf_size, columns, leaf_size), bf16),
                pltpu.VMEM((columns, tests), f32),
            ],
        ),
        compiler_params=pltpu.CompilerParams(vmem_limit_bytes=24 << 20),
        name="posterior_mean",
    )(slots, *whole, in_hbm(early), in_hbm(late), last, far)


def exchange(value, axes):
    return lax.all_to_all(value, axes, 0, 0)


def gathered(value, axes):
    count = lax.axis_size(axes)
    return exchange(jnp.broadcast_to(value[None], (count,) + value.shape), axes)


def tie(*values):
    return lax.optimization_barrier(values)


def shards(
    targets,
    tree_order,
    leaf_inverse,
    cluster_basis,
    coupling,
    train_coords,
    test_coords,
    test_basis,
    near_leaves,
):
    columns, points = targets.shape
    leaf_count, leaf_size = leaf_inverse.shape[:2]
    all_levels, rank = cluster_basis.shape[:2]
    local_levels = leaf_count.bit_length() - 1
    low_count = lax.axis_size(low_axes)
    high_count = lax.axis_size("z")
    low_levels = low_count.bit_length() - 1
    low = lax.axis_index(low_axes)
    high = lax.axis_index("z")
    panels = low_count * high_count
    width = (all_levels - local_levels) * rank
    low_width = low_levels * rank
    part = width // low_count
    share = columns // low_count
    place = jnp.stack([low, high]).astype(jnp.int32)
    position = high * low_count + low
    basis = cluster_basis.reshape(all_levels * rank, points)
    mixers = coupling[0]
    half_slots = near_leaves.shape[1] // 2

    def mixer(*refs):
        mixer_body(*refs, local_levels=local_levels, part=part)

    effect = whole_call(
        mixer, jax.ShapeDtypeStruct((low_count, 2 * part, width), f32), "mixer", limit=None
    )(basis, mixers)
    effect, train_coords = tie(effect, train_coords)
    spread = exchange(effect, low_axes)

    def featured(*refs):
        points_body(*refs, scale=3.0 / length_scale**2)

    features = jax.ShapeDtypeStruct((16, points), bf16)
    train_rows, test_rows = whole_call(
        featured, [features] * 2, "points", scratch=[pltpu.VMEM((16, points), f32)]
    )(train_coords, test_coords)
    forward = [(i, i + 1) for i in range(panels - 1)]
    backward = [(i + 1, i) for i in range(panels - 1)]
    train_rows, tree_order = tie(train_rows, tree_order)

    state, terms = whole_call(
        local_body,
        [
            jax.ShapeDtypeStruct((columns, points), f32),
            jax.ShapeDtypeStruct((columns, width), f32),
        ],
        "local",
        limit=None,
    )(targets, tree_order, leaf_inverse, basis, mixers)
    terms, spread = tie(terms, spread)

    slots = near_leaves[0] - (position - 1) * leaf_count
    total = jnp.sum(spread, axis=0)[:, low_width:]
    early_slots, train_rows, total = tie(slots[:half_slots], train_rows, total)
    sides = (
        lax.ppermute(train_rows, panel_axes, forward),
        train_rows,
        lax.ppermute(train_rows, panel_axes, backward),
    )
    high_spread = gathered(total, "z")
    early = distance_kernel(early_slots, sides, test_rows, leaf_size, "near_early")
    early, high_spread = tie(early, high_spread)

    def operator(*refs):
        operator_body(*refs, rank=rank)

    operators = whole_call(
        operator, jax.ShapeDtypeStruct((low_count, 3 * part, width), bf16), "operator", 1
    )(place, spread, high_spread)
    late_slots, operators = tie(slots[half_slots:-1], operators)
    operators = exchange(operators, low_axes)
    late = distance_kernel(late_slots, sides, test_rows, leaf_size, "near_late")
    late, operators = tie(late, operators)

    def eliminate(*refs):
        eliminate_body(*refs, rank=rank)

    own_terms = whole_call(
        eliminate, jax.ShapeDtypeStruct((low_count, share, width), f32), "eliminate"
    )(terms, operators)
    spread = exchange(own_terms, low_axes)
    high_spread = gathered(jnp.sum(spread, axis=0)[:, low_width:], "z")

    def subtree(*refs):
        sums_body(*refs, rank=rank)

    sums = whole_call(
        subtree, jax.ShapeDtypeStruct((low_count, 2 * share, width), f32), "subtree", 1
    )(place, spread, high_spread)
    sums = exchange(sums, low_axes)

    def weigh(*refs):
        weights_body(*refs, local_levels=local_levels)

    weights, joined = whole_call(
        weigh,
        [
            jax.ShapeDtypeStruct((columns, points), bf16),
            jax.ShapeDtypeStruct((2 * columns, width), f32),
        ],
        "weights",
    )(sums, state, basis, mixers)
    last_slot, weights = tie(slots[-1:], weights)
    last = distance_kernel(
        last_slot, sides, test_rows, leaf_size, "near_last", jax.ShapeDtypeStruct
    )
    before = lax.ppermute(weights, panel_axes, forward)
    after = lax.ppermute(weights, panel_axes, backward)
    factor = 2.0 / math.sqrt(near_leaves.shape[1] * leaf_size)

    def distant(*refs):
        far_body(*refs, rank=rank, factor=factor)

    far = whole_call(distant, jax.ShapeDtypeStruct((columns, points), f32), "far")(
        joined, operators, test_basis.reshape(width, -1)
    )
    return mean_kernel(slots, before, weights, after, early, late, last, far, factor)


def solution(mesh):
    grp, leaf, sub = (mesh.shape[name] for name in ("grp", "leaf", "sub"))
    split = Mesh(mesh.devices.reshape(grp, leaf // 2, 2, sub), ("grp",) + panel_axes)
    every = ("grp",) + panel_axes
    return jax.shard_map(
        shards,
        mesh=split,
        in_specs=(
            P(None, every),
            P(every, None),
            P(every, None, None),
            P(None, None, every),
            P(every, None, None, None),
            P(None, every),
            P(None, every),
            P(None, None, every),
            P(every, None),
        ),
        out_specs=P(None, every),
        check_vma=False,
    )
```

```python
import math

import jax
import jax.numpy as jnp
from jax import lax
from jax.experimental import pallas as pl
from jax.experimental.pallas import tpu as pltpu
from jax.sharding import Mesh
from jax.sharding import PartitionSpec as P

length_scale = 0.5
highest = lax.Precision.HIGHEST
low_axes = ("core", "sub")
panel_axes = ("z", "core", "sub")
f32 = jnp.float32
bf16 = jnp.bfloat16
rows_by_columns = (((1,), (0,)), ((), ()))
rows_by_rows = (((1,), (1,)), ((), ()))
columns_by_columns = (((0,), (0,)), ((), ()))


def thirds(value):
    high = value.astype(bf16)
    rest = value - high.astype(f32)
    middle = rest.astype(bf16)
    low = (rest - middle.astype(f32)).astype(bf16)
    return high, middle, low


def wide_dot(left, right, dims):
    rows = left.shape[0]
    stacked = jnp.concatenate(thirds(left), axis=0)
    product = lax.dot_general(stacked, right, dims, preferred_element_type=f32)
    return product[:rows] + product[rows : 2 * rows] + product[2 * rows :]


def full_dot(left, right, dims=rows_by_columns):
    return lax.dot_general(left, right, dims, precision=highest, preferred_element_type=f32)


def whole_call(body, out_shape, name, scalars=0, scratch=(), limit=20 << 20):
    def call(*operands):
        specs = [
            pl.BlockSpec(memory_space=pltpu.SMEM if i < scalars else pltpu.VMEM)
            for i in range(len(operands))
        ]
        single = not isinstance(out_shape, (list, tuple))
        out_specs = pl.BlockSpec(memory_space=pltpu.VMEM)
        return pl.pallas_call(
            body,
            out_shape=out_shape,
            in_specs=specs,
            out_specs=out_specs if single else [out_specs] * len(out_shape),
            scratch_shapes=list(scratch),
            name=name,
            compiler_params=pltpu.CompilerParams(vmem_limit_bytes=limit),
        )(*operands)

    return call


def points_body(train_ref, test_ref, left_ref, right_ref, rows_ref, *, scale):
    dims, count = train_ref.shape
    ones = jnp.ones((1, count), f32)
    for ref, out_ref in ((train_ref, left_ref), (test_ref, right_ref)):
        exact = ref[...].astype(f32)
        norms = scale * jnp.sum(exact * exact, axis=0, keepdims=True)
        norms = [piece.astype(f32) for piece in thirds(norms)]
        if out_ref is left_ref:
            rows = [exact[axis : axis + 1] for axis in range(dims)] * 3 + norms + [ones] * 3
        else:
            pieces = [piece.astype(f32) for piece in thirds(-2.0 * scale * exact)]
            rows = [piece[axis : axis + 1] for piece in pieces for axis in range(dims)]
            rows = rows + [ones] * 3 + norms
        rows_ref[...] = jnp.zeros_like(rows_ref)
        for place, row in enumerate(rows):
            rows_ref[place : place + 1, :] = row
        out_ref[...] = rows_ref[...].astype(bf16)


def mixer_body(basis_ref, coupling_ref, out_ref, *, local_levels, part):
    rank = coupling_ref.shape[1]
    width = basis_ref.shape[0] - local_levels * rank
    points = basis_ref.shape[1]
    basis = basis_ref[local_levels * rank :, :]
    gram = lax.dot_general(basis, basis, rows_by_rows, preferred_element_type=f32)
    level = lax.broadcasted_iota(jnp.int32, (1, width), 1) // rank
    gram = gram * (lax.exp2(-0.5 * level.astype(f32)) / math.sqrt(points))
    for depth in range(width // rank):
        piece = gram[depth * rank : (depth + 1) * rank, :]
        product = full_dot(coupling_ref[local_levels + depth], piece, columns_by_columns)
        for half in range(2):
            for block in range(rank // part):
                start = half * rank + block * part
                out_ref[depth * (rank // part) + block, half * part : (half + 1) * part, :] = (
                    product[start : start + part, :]
                )


def local_body(targets_ref, order_ref, inverse_ref, basis_ref, coupling_ref, state_ref, terms_ref):
    columns, points = targets_ref.shape
    leaf_count, leaf_size, _ = inverse_ref.shape
    rank = coupling_ref.shape[1]
    local_levels = leaf_count.bit_length() - 1
    place = lax.broadcasted_iota(jnp.int32, (points, leaf_size), 0)
    for leaf in range(leaf_count):
        lanes = slice(leaf * leaf_size, (leaf + 1) * leaf_size)
        chosen = jnp.where(place == order_ref[:, lanes], 1.0, 0.0).astype(bf16)
        block = jnp.dot(targets_ref[...], chosen, preferred_element_type=f32).astype(bf16)
        state_ref[:, lanes] = lax.dot_general(
            block, inverse_ref[leaf], rows_by_rows, preferred_element_type=f32
        )
    for level in range(local_levels):
        child = leaf_size << level
        count = points // child
        mixers = coupling_ref[level]
        bases = [
            basis_ref[level * rank : (level + 1) * rank, c * child : (c + 1) * child]
            for c in range(count)
        ]
        sums = [
            wide_dot(state_ref[:, c * child : (c + 1) * child], bases[c], rows_by_rows)
            / math.sqrt(child)
            for c in range(count)
        ]
        for c in range(count):
            joined = jnp.concatenate([sums[c], sums[c ^ 1]], axis=1)
            mixed = full_dot(joined, mixers, rows_by_rows)
            lanes = slice(c * child, (c + 1) * child)
            state_ref[:, lanes] = state_ref[:, lanes] - wide_dot(mixed, bases[c], rows_by_columns)
    width = terms_ref.shape[1]
    level = lax.broadcasted_iota(jnp.int32, (1, width), 1) // rank
    scale = lax.exp2(-0.5 * level.astype(f32)) / math.sqrt(points)
    terms_ref[...] = (
        wide_dot(state_ref[...], basis_ref[local_levels * rank :, :], rows_by_rows) * scale
    )


def distance_body(slots_ref, before_ref, mine_ref, after_ref, test_ref, out_ref, train_ref):
    leaf = slots_ref[pl.program_id(0)]
    leaf_size = train_ref.shape[1]
    leaf_count = mine_ref.shape[1] // leaf_size
    for side, ref in enumerate((before_ref, mine_ref, after_ref)):

        @pl.when(leaf // leaf_count == side)
        def _(ref=ref):
            start = pl.multiple_of((leaf % leaf_count) * leaf_size, leaf_size)
            train_ref[...] = ref[:, pl.ds(start, leaf_size)]

    train = train_ref[...]
    step = 256
    for start in range(0, test_ref.shape[1], step):
        squared = lax.dot_general(
            train, test_ref[:, start : start + step], columns_by_columns,
            preferred_element_type=f32,
        )
        squared = jnp.maximum(squared, 1e-20)
        scaled = squared * lax.rsqrt(squared)
        out_ref[0, :, start : start + step] = ((1.0 + scaled) * jnp.exp(-scaled)).astype(bf16)


def distance_kernel(
    slots, sides, test_features, leaf_size, name, total, first=0, buffer=None, store=pltpu.HBM
):
    tests = test_features.shape[1]
    operands = (*sides, test_features)
    held = () if buffer is None else (buffer,)

    def body(slots_ref, *refs):
        distance_body(slots_ref, *refs[len(held) :])

    return pl.pallas_call(
        body,
        out_shape=store((total, leaf_size, tests), bf16),
        grid_spec=pltpu.PrefetchScalarGridSpec(
            num_scalar_prefetch=1,
            grid=(slots.shape[0],),
            in_specs=[pl.BlockSpec(memory_space=pl.ANY) for _ in held]
            + [pl.BlockSpec(a.shape, lambda i, s: (0, 0)) for a in operands],
            out_specs=pl.BlockSpec((1, leaf_size, tests), lambda i, s: (first + i, 0, 0)),
            scratch_shapes=[pltpu.VMEM((sides[0].shape[0], leaf_size), bf16)],
        ),
        compiler_params=pltpu.CompilerParams(vmem_limit_bytes=24 << 20),
        input_output_aliases={1: 0} if held else {},
        name=name,
    )(slots, *held, *operands)


def node_sums(members, levels):
    sums = [members]
    for _ in range(levels):
        last = sums[-1]
        sums.append([last[i] + last[i + 1] for i in range(0, len(last), 2)])
    return sums


def chain_sums(values, position, levels):
    tree = node_sums(values, levels)
    own, sibling = [], []
    for level in range(levels):
        nodes = tree[level]
        mine = position >> level
        first, second = nodes[0], nodes[1]
        for node in range(2, len(nodes), 2):
            here = (mine >> 1) == (node >> 1)
            first = jnp.where(here, nodes[node], first)
            second = jnp.where(here, nodes[node + 1], second)
        right = (mine & 1) == 1
        own.append(jnp.where(right, second, first))
        sibling.append(jnp.where(right, first, second))
    return own, sibling


def operator_body(place_ref, spread_ref, high_ref, out_ref, *, rank):
    low_count, rows, width = spread_ref.shape
    part = rows // 2
    high_count, _, high_width = high_ref.shape
    low_width = width - high_width
    low_levels = low_count.bit_length() - 1
    high_levels = high_count.bit_length() - 1
    row_level = place_ref[0] * part // rank
    lane_level = lax.broadcasted_iota(jnp.int32, (part, width), 1) // rank
    pair_level = jnp.minimum(lane_level, row_level)
    upper = pair_level >= low_levels
    below = lane_level < row_level
    equal = lane_level == row_level
    blank = jnp.zeros((part, low_width), f32)
    trees = []
    highs = []
    for half in range(2):
        rows_here = slice(half * part, (half + 1) * part)
        trees.append(node_sums([spread_ref[p, rows_here, :] for p in range(low_count)], low_levels))
        own, sibling = chain_sums(
            [high_ref[p, rows_here, :] for p in range(high_count)], place_ref[1], high_levels
        )
        picks = []
        for values in (own, sibling):
            pick = values[0]
            for level in range(1, high_levels):
                pick = jnp.where(
                    pair_level[:, low_width:] == low_levels + level, values[level], pick
                )
            picks.append(jnp.concatenate([blank, pick], axis=1))
        highs.append(picks)
    for p in range(low_count):
        own, sibling = [], []
        for half in range(2):
            mine, other = highs[half]
            for level in range(low_levels):
                chosen = pair_level == level
                mine = jnp.where(chosen, trees[half][level][p >> level], mine)
                other = jnp.where(chosen, trees[half][level][(p >> level) ^ 1], other)
            own.append(mine)
            sibling.append(other)
        ahead = own[0] + sibling[1]
        first = jnp.where(below, sibling[0], jnp.where(equal, sibling[1], ahead))
        high = first.astype(bf16)
        out_ref[p, :part, :] = high
        out_ref[p, part : 2 * part, :] = (first - high.astype(f32)).astype(bf16)
        out_ref[p, 2 * part :, :] = jnp.where(equal, sibling[0], sibling[1]).astype(bf16)


def operators_of(ref, rank):
    count, rows, width = ref.shape
    part = rows // 3
    first, rest, second = (
        ref[:, i * part : (i + 1) * part, :].reshape(count * part, width).astype(f32)
        for i in range(3)
    )
    first = first + rest
    row_level = lax.broadcasted_iota(jnp.int32, (width, width), 0) // rank
    lane_level = lax.broadcasted_iota(jnp.int32, (width, width), 1) // rank
    return first, second, lane_level > row_level


def eliminate_body(terms_ref, operators_ref, out_ref, *, rank):
    columns, width = terms_ref.shape
    count, share, _ = out_ref.shape
    first, _, ahead = operators_of(operators_ref, rank)
    feed = jnp.where(ahead, first, 0.0)
    half = width // 2

    def solve(value, square):
        double = full_dot(square, square)
        value = value - full_dot(value, square)
        return value + full_dot(value, double)

    early = solve(terms_ref[:, :half], feed[:half, :half])
    late = terms_ref[:, half:] - full_dot(early, feed[:half, half:])
    late = solve(late, feed[half:, half:])
    for j in range(count):
        rows = slice(j * share, (j + 1) * share)
        out_ref[j, :, :half] = early[rows, :]
        out_ref[j, :, half:] = late[rows, :]


def sums_body(place_ref, spread_ref, high_ref, out_ref, *, rank):
    low_count, share, width = spread_ref.shape
    high_count, _, high_width = high_ref.shape
    low_width = width - high_width
    low_levels = low_count.bit_length() - 1
    high_levels = high_count.bit_length() - 1
    lane_level = lax.broadcasted_iota(jnp.int32, (share, width), 1) // rank
    tree = node_sums([spread_ref[p] for p in range(low_count)], low_levels)
    blank = jnp.zeros((share, low_width), f32)
    highs = []
    for values in chain_sums([high_ref[p] for p in range(high_count)], place_ref[1], high_levels):
        pick = values[0]
        for level in range(1, high_levels):
            pick = jnp.where(lane_level[:, low_width:] == low_levels + level, values[level], pick)
        highs.append(jnp.concatenate([blank, pick], axis=1))
    for p in range(low_count):
        mine, other = highs
        for level in range(low_levels):
            chosen = lane_level == level
            mine = jnp.where(chosen, tree[level][p >> level], mine)
            other = jnp.where(chosen, tree[level][(p >> level) ^ 1], other)
        out_ref[p, :share, :] = mine
        out_ref[p, share:, :] = other


def weights_body(sums_ref, state_ref, basis_ref, coupling_ref, weights_ref, joined_ref, *, local_levels):
    count, rows, width = sums_ref.shape
    share = rows // 2
    columns = count * share
    rank = coupling_ref.shape[1]
    for j in range(count):
        joined_ref[j * share : (j + 1) * share, :] = sums_ref[j, :share, :]
        joined_ref[columns + j * share : columns + (j + 1) * share, :] = sums_ref[j, share:, :]
    pieces = []
    for level in range(width // rank):
        lanes = slice(level * rank, (level + 1) * rank)
        joined = jnp.concatenate(
            [joined_ref[:columns, lanes], joined_ref[columns:, lanes]], axis=1
        )
        pieces.append(full_dot(joined, coupling_ref[local_levels + level], rows_by_rows))
    mixed = jnp.concatenate(pieces, axis=1)
    update = wide_dot(mixed, basis_ref[local_levels * rank :, :], rows_by_columns)
    weights_ref[...] = (state_ref[...] - update).astype(bf16)


def far_body(joined_ref, operators_ref, test_ref, out_ref, *, rank, factor):
    columns = out_ref.shape[0]
    first, second, ahead = operators_of(operators_ref, rank)
    own = joined_ref[:columns, :]
    sibling = joined_ref[columns:, :]
    far = (
        sibling
        - full_dot(own, jnp.where(ahead, 0.0, first))
        - full_dot(sibling, jnp.where(ahead, 0.0, second))
    )
    out_ref[...] = wide_dot(far, test_ref[...], rows_by_columns) / factor


def mean_body(
    slots_ref, before_ref, mine_ref, after_ref, values_ref, last_ref, far_ref,
    out_ref, window_ref, near_ref, *, leaf_size, factor,
):
    step = pl.program_id(0)
    steps = pl.num_programs(0)
    leaf_count = mine_ref.shape[1] // leaf_size

    def part_of(slot, values):
        return jnp.dot(window_ref[slots_ref[slot]], values, preferred_element_type=f32)

    @pl.when(step == 0)
    def _():
        for side, ref in enumerate((before_ref, mine_ref, after_ref)):
            for leaf in range(leaf_count):
                window_ref[side * leaf_count + leaf] = ref[
                    :, leaf * leaf_size : (leaf + 1) * leaf_size
                ]
        near_ref[...] = far_ref[...]
        for place in range(last_ref.shape[0]):
            near_ref[...] += part_of(steps + place, last_ref[place])

    near_ref[...] += part_of(step, values_ref[0])

    @pl.when(step == steps - 1)
    def _():
        out_ref[...] = (near_ref[...] * factor).astype(bf16)


def mean_kernel(slots, before, mine, after, values, last, far, factor):
    stored, leaf_size, tests = values.shape
    columns, points = mine.shape
    whole = [before, mine, after]

    def fixed(array):
        return pl.BlockSpec(array.shape, lambda i, s: (0,) * array.ndim)

    def body(*refs):
        mean_body(*refs, leaf_size=leaf_size, factor=factor)

    return pl.pallas_call(
        body,
        out_shape=jax.ShapeDtypeStruct((columns, tests), bf16),
        grid_spec=pltpu.PrefetchScalarGridSpec(
            num_scalar_prefetch=1,
            grid=(stored,),
            in_specs=[fixed(a) for a in whole]
            + [
                pl.BlockSpec((1, leaf_size, tests), lambda i, s: (i, 0, 0)),
                pl.BlockSpec(memory_space=pltpu.VMEM),
                fixed(far),
            ],
            out_specs=pl.BlockSpec((columns, tests), lambda i, s: (0, 0)),
            scratch_shapes=[
                pltpu.VMEM((3 * points // leaf_size, columns, leaf_size), bf16),
                pltpu.VMEM((columns, tests), f32),
            ],
        ),
        compiler_params=pltpu.CompilerParams(vmem_limit_bytes=24 << 20),
        name="posterior_mean",
    )(slots, *whole, pltpu.with_memory_space_constraint(values, pltpu.HBM), last, far)


def exchange(value, axes):
    return lax.all_to_all(value, axes, 0, 0)


def gathered(value, axes):
    count = lax.axis_size(axes)
    return exchange(jnp.broadcast_to(value[None], (count,) + value.shape), axes)


def tie(*values):
    return lax.optimization_barrier(values)


def shards(
    targets,
    tree_order,
    leaf_inverse,
    cluster_basis,
    coupling,
    train_coords,
    test_coords,
    test_basis,
    near_leaves,
):
    columns, points = targets.shape
    leaf_count, leaf_size = leaf_inverse.shape[:2]
    all_levels, rank = cluster_basis.shape[:2]
    local_levels = leaf_count.bit_length() - 1
    low_count = lax.axis_size(low_axes)
    high_count = lax.axis_size("z")
    low_levels = low_count.bit_length() - 1
    low = lax.axis_index(low_axes)
    high = lax.axis_index("z")
    panels = low_count * high_count
    width = (all_levels - local_levels) * rank
    low_width = low_levels * rank
    part = width // low_count
    share = columns // low_count
    place = jnp.stack([low, high]).astype(jnp.int32)
    position = high * low_count + low
    basis = cluster_basis.reshape(all_levels * rank, points)
    mixers = coupling[0]
    slot_count = near_leaves.shape[1]
    early_count, last_count = slot_count // 4, slot_count // 4
    stored = slot_count - last_count

    def mixer(*refs):
        mixer_body(*refs, local_levels=local_levels, part=part)

    effect = whole_call(
        mixer, jax.ShapeDtypeStruct((low_count, 2 * part, width), f32), "mixer", limit=None
    )(basis, mixers)
    effect, train_coords = tie(effect, train_coords)
    spread = exchange(effect, low_axes)

    def featured(*refs):
        points_body(*refs, scale=3.0 / length_scale**2)

    features = jax.ShapeDtypeStruct((16, points), bf16)
    train_rows, test_rows = whole_call(
        featured, [features] * 2, "points", scratch=[pltpu.VMEM((16, points), f32)]
    )(train_coords, test_coords)
    forward = [(i, i + 1) for i in range(panels - 1)]
    backward = [(i + 1, i) for i in range(panels - 1)]
    train_rows, tree_order = tie(train_rows, tree_order)

    state, terms = whole_call(
        local_body,
        [
            jax.ShapeDtypeStruct((columns, points), f32),
            jax.ShapeDtypeStruct((columns, width), f32),
        ],
        "local",
        limit=None,
    )(targets, tree_order, leaf_inverse, basis, mixers)
    terms, spread = tie(terms, spread)

    slots = near_leaves[0] - (position - 1) * leaf_count
    total = jnp.sum(spread, axis=0)[:, low_width:]
    early_slots, train_rows, total = tie(slots[:early_count], train_rows, total)
    sides = (
        lax.ppermute(train_rows, panel_axes, forward),
        train_rows,
        lax.ppermute(train_rows, panel_axes, backward),
    )
    high_spread = gathered(total, "z")
    early = distance_kernel(early_slots, sides, test_rows, leaf_size, "near_early", stored)
    early, high_spread = tie(early, high_spread)

    def operator(*refs):
        operator_body(*refs, rank=rank)

    operators = whole_call(
        operator, jax.ShapeDtypeStruct((low_count, 3 * part, width), bf16), "operator", 1
    )(place, spread, high_spread)
    late_slots, operators = tie(slots[early_count:stored], operators)
    operators = exchange(operators, low_axes)
    late = distance_kernel(
        late_slots, sides, test_rows, leaf_size, "near_late", stored, early_count, early
    )
    late, operators = tie(late, operators)

    def eliminate(*refs):
        eliminate_body(*refs, rank=rank)

    own_terms = whole_call(
        eliminate, jax.ShapeDtypeStruct((low_count, share, width), f32), "eliminate"
    )(terms, operators)
    spread = exchange(own_terms, low_axes)
    high_spread = gathered(jnp.sum(spread, axis=0)[:, low_width:], "z")

    def subtree(*refs):
        sums_body(*refs, rank=rank)

    sums = whole_call(
        subtree, jax.ShapeDtypeStruct((low_count, 2 * share, width), f32), "subtree", 1
    )(place, spread, high_spread)
    sums = exchange(sums, low_axes)

    def weigh(*refs):
        weights_body(*refs, local_levels=local_levels)

    weights, joined = whole_call(
        weigh,
        [
            jax.ShapeDtypeStruct((columns, points), bf16),
            jax.ShapeDtypeStruct((2 * columns, width), f32),
        ],
        "weights",
    )(sums, state, basis, mixers)
    last_slots, weights = tie(slots[stored:], weights)
    last = distance_kernel(
        last_slots, sides, test_rows, leaf_size, "near_last", last_count,
        store=jax.ShapeDtypeStruct,
    )
    before = lax.ppermute(weights, panel_axes, forward)
    after = lax.ppermute(weights, panel_axes, backward)
    factor = 2.0 / math.sqrt(near_leaves.shape[1] * leaf_size)

    def distant(*refs):
        far_body(*refs, rank=rank, factor=factor)

    far = whole_call(distant, jax.ShapeDtypeStruct((columns, points), f32), "far")(
        joined, operators, test_basis.reshape(width, -1)
    )
    return mean_kernel(slots, before, weights, after, late, last, far, factor)


def solution(mesh):
    grp, leaf, sub = (mesh.shape[name] for name in ("grp", "leaf", "sub"))
    split = Mesh(mesh.devices.reshape(grp, leaf // 2, 2, sub), ("grp",) + panel_axes)
    every = ("grp",) + panel_axes
    return jax.shard_map(
        shards,
        mesh=split,
        in_specs=(
            P(None, every),
            P(every, None),
            P(every, None, None),
            P(None, None, every),
            P(every, None, None, None),
            P(None, every),
            P(None, every),
            P(None, None, every),
            P(every, None),
        ),
        out_specs=P(None, every),
        check_vma=False,
    )
```

```python
import math

import jax
import jax.numpy as jnp
from jax import lax
from jax.experimental import pallas as pl
from jax.experimental.pallas import tpu as pltpu
from jax.sharding import Mesh
from jax.sharding import PartitionSpec as P

length_scale = 0.5
highest = lax.Precision.HIGHEST
low_axes = ("core", "sub")
panel_axes = ("z", "core", "sub")
f32 = jnp.float32
bf16 = jnp.bfloat16
rows_by_columns = (((1,), (0,)), ((), ()))
rows_by_rows = (((1,), (1,)), ((), ()))
columns_by_columns = (((0,), (0,)), ((), ()))


def thirds(value):
    high = value.astype(bf16)
    rest = value - high.astype(f32)
    middle = rest.astype(bf16)
    low = (rest - middle.astype(f32)).astype(bf16)
    return high, middle, low


def wide_dot(left, right, dims):
    rows = left.shape[0]
    stacked = jnp.concatenate(thirds(left), axis=0)
    product = lax.dot_general(stacked, right, dims, preferred_element_type=f32)
    return product[:rows] + product[rows : 2 * rows] + product[2 * rows :]


def full_dot(left, right, dims=rows_by_columns):
    return lax.dot_general(left, right, dims, precision=highest, preferred_element_type=f32)


def whole_call(body, out_shape, name, scalars=0, scratch=(), limit=20 << 20):
    def call(*operands):
        specs = [
            pl.BlockSpec(memory_space=pltpu.SMEM if i < scalars else pltpu.VMEM)
            for i in range(len(operands))
        ]
        single = not isinstance(out_shape, (list, tuple))
        out_specs = pl.BlockSpec(memory_space=pltpu.VMEM)
        return pl.pallas_call(
            body,
            out_shape=out_shape,
            in_specs=specs,
            out_specs=out_specs if single else [out_specs] * len(out_shape),
            scratch_shapes=list(scratch),
            name=name,
            compiler_params=pltpu.CompilerParams(vmem_limit_bytes=limit),
        )(*operands)

    return call


def points_body(train_ref, test_ref, left_ref, right_ref, rows_ref, *, scale):
    dims, count = train_ref.shape
    ones = jnp.ones((1, count), f32)
    for ref, out_ref in ((train_ref, left_ref), (test_ref, right_ref)):
        exact = ref[...].astype(f32)
        norms = scale * jnp.sum(exact * exact, axis=0, keepdims=True)
        norms = [piece.astype(f32) for piece in thirds(norms)]
        if out_ref is left_ref:
            rows = [exact[axis : axis + 1] for axis in range(dims)] * 3 + norms + [ones] * 3
        else:
            pieces = [piece.astype(f32) for piece in thirds(-2.0 * scale * exact)]
            rows = [piece[axis : axis + 1] for piece in pieces for axis in range(dims)]
            rows = rows + [ones] * 3 + norms
        rows_ref[...] = jnp.zeros_like(rows_ref)
        for place, row in enumerate(rows):
            rows_ref[place : place + 1, :] = row
        out_ref[...] = rows_ref[...].astype(bf16)


def mixer_body(basis_ref, coupling_ref, out_ref, *, local_levels):
    rank = coupling_ref.shape[1]
    width = basis_ref.shape[0] - local_levels * rank
    points = basis_ref.shape[1]
    basis = basis_ref[local_levels * rank :, :]
    gram = lax.dot_general(basis, basis, rows_by_rows, preferred_element_type=f32)
    level = lax.broadcasted_iota(jnp.int32, (1, width), 1) // rank
    gram = gram * (lax.exp2(-0.5 * level.astype(f32)) / math.sqrt(points))
    piece = out_ref.shape[1] // 4
    for depth in range(width // rank):
        rows = gram[depth * rank : (depth + 1) * rank, :]
        product = full_dot(coupling_ref[local_levels + depth], rows, columns_by_columns)
        upper, group = divmod(depth, width // rank // 2)
        for half in range(2):
            for block in range(rank // piece):
                start = half * rank + block * piece
                row = (2 * half + upper) * piece
                out_ref[group * (rank // piece) + block, row : row + piece, :] = product[
                    start : start + piece, :
                ]


def local_body(targets_ref, order_ref, inverse_ref, basis_ref, coupling_ref, state_ref, terms_ref):
    columns, points = targets_ref.shape
    leaf_count, leaf_size, _ = inverse_ref.shape
    rank = coupling_ref.shape[1]
    local_levels = leaf_count.bit_length() - 1
    place = lax.broadcasted_iota(jnp.int32, (points, leaf_size), 0)
    for leaf in range(leaf_count):
        lanes = slice(leaf * leaf_size, (leaf + 1) * leaf_size)
        chosen = jnp.where(place == order_ref[:, lanes], 1.0, 0.0).astype(bf16)
        block = jnp.dot(targets_ref[...], chosen, preferred_element_type=f32).astype(bf16)
        state_ref[:, lanes] = lax.dot_general(
            block, inverse_ref[leaf], rows_by_rows, preferred_element_type=f32
        )
    for level in range(local_levels):
        child = leaf_size << level
        count = points // child
        mixers = coupling_ref[level]
        bases = [
            basis_ref[level * rank : (level + 1) * rank, c * child : (c + 1) * child]
            for c in range(count)
        ]
        sums = [
            wide_dot(state_ref[:, c * child : (c + 1) * child], bases[c], rows_by_rows)
            / math.sqrt(child)
            for c in range(count)
        ]
        for c in range(count):
            joined = jnp.concatenate([sums[c], sums[c ^ 1]], axis=1)
            mixed = full_dot(joined, mixers, rows_by_rows)
            lanes = slice(c * child, (c + 1) * child)
            state_ref[:, lanes] = state_ref[:, lanes] - wide_dot(mixed, bases[c], rows_by_columns)
    width = terms_ref.shape[1]
    level = lax.broadcasted_iota(jnp.int32, (1, width), 1) // rank
    scale = lax.exp2(-0.5 * level.astype(f32)) / math.sqrt(points)
    terms_ref[...] = (
        wide_dot(state_ref[...], basis_ref[local_levels * rank :, :], rows_by_rows) * scale
    )


def distance_body(slots_ref, before_ref, mine_ref, after_ref, test_ref, out_ref, train_ref):
    leaf = slots_ref[pl.program_id(0)]
    leaf_size = train_ref.shape[1]
    leaf_count = mine_ref.shape[1] // leaf_size
    for side, ref in enumerate((before_ref, mine_ref, after_ref)):

        @pl.when(leaf // leaf_count == side)
        def _(ref=ref):
            start = pl.multiple_of((leaf % leaf_count) * leaf_size, leaf_size)
            train_ref[...] = ref[:, pl.ds(start, leaf_size)]

    train = train_ref[...]
    step = 256
    for start in range(0, test_ref.shape[1], step):
        squared = lax.dot_general(
            train, test_ref[:, start : start + step], columns_by_columns,
            preferred_element_type=f32,
        )
        squared = jnp.maximum(squared, 1e-20)
        scaled = squared * lax.rsqrt(squared)
        out_ref[0, :, start : start + step] = ((1.0 + scaled) * jnp.exp(-scaled)).astype(bf16)


def distance_kernel(slots, sides, test_features, leaf_size, name, store):
    tests = test_features.shape[1]
    operands = (*sides, test_features)
    return pl.pallas_call(
        distance_body,
        out_shape=store((slots.shape[0], leaf_size, tests), bf16),
        grid_spec=pltpu.PrefetchScalarGridSpec(
            num_scalar_prefetch=1,
            grid=(slots.shape[0],),
            in_specs=[pl.BlockSpec(a.shape, lambda i, s: (0, 0)) for a in operands],
            out_specs=pl.BlockSpec((1, leaf_size, tests), lambda i, s: (i, 0, 0)),
            scratch_shapes=[pltpu.VMEM((sides[0].shape[0], leaf_size), bf16)],
        ),
        compiler_params=pltpu.CompilerParams(vmem_limit_bytes=24 << 20),
        name=name,
    )(slots, *operands)


def node_sums(members, levels):
    sums = [members]
    for _ in range(levels):
        last = sums[-1]
        sums.append([last[i] + last[i + 1] for i in range(0, len(last), 2)])
    return sums


def chain_sums(values, position, levels):
    tree = node_sums(values, levels)
    own, sibling = [], []
    for level in range(levels):
        nodes = tree[level]
        mine = position >> level
        first, second = nodes[0], nodes[1]
        for node in range(2, len(nodes), 2):
            here = (mine >> 1) == (node >> 1)
            first = jnp.where(here, nodes[node], first)
            second = jnp.where(here, nodes[node + 1], second)
        right = (mine & 1) == 1
        own.append(jnp.where(right, second, first))
        sibling.append(jnp.where(right, first, second))
    return own, sibling


def operator_body(place_ref, spread_ref, high_ref, out_ref, *, rank):
    low_count, rows, width = spread_ref.shape
    part = rows // 2
    high_count, _, high_width = high_ref.shape
    low_width = width - high_width
    low_levels = low_count.bit_length() - 1
    high_levels = high_count.bit_length() - 1
    piece = part // 2
    row = lax.broadcasted_iota(jnp.int32, (part, width), 0)
    row_level = place_ref[0] * piece // rank + low_levels * (row // piece)
    lane_level = lax.broadcasted_iota(jnp.int32, (part, width), 1) // rank
    pair_level = jnp.minimum(lane_level, row_level)
    below = lane_level < row_level
    equal = lane_level == row_level
    blank = jnp.zeros((piece, low_width), f32)
    trees = []
    highs = []
    for half in range(2):
        rows_here = slice(half * part, (half + 1) * part)
        trees.append(node_sums([spread_ref[p, rows_here, :] for p in range(low_count)], low_levels))
        own, sibling = chain_sums(
            [high_ref[p, half * piece : (half + 1) * piece, :] for p in range(high_count)],
            place_ref[1],
            high_levels,
        )
        picks = []
        for values in (own, sibling):
            pick = values[0]
            for level in range(1, high_levels):
                pick = jnp.where(
                    pair_level[piece:, low_width:] == low_levels + level, values[level], pick
                )
            pick = jnp.concatenate([blank, pick], axis=1)
            picks.append(jnp.concatenate([jnp.zeros_like(pick), pick], axis=0))
        highs.append(picks)
    for p in range(low_count):
        own, sibling = [], []
        for half in range(2):
            mine, other = highs[half]
            for level in range(low_levels):
                chosen = pair_level == level
                mine = jnp.where(chosen, trees[half][level][p >> level], mine)
                other = jnp.where(chosen, trees[half][level][(p >> level) ^ 1], other)
            own.append(mine)
            sibling.append(other)
        ahead = own[0] + sibling[1]
        first = jnp.where(below, sibling[0], jnp.where(equal, sibling[1], ahead))
        high = first.astype(bf16)
        out_ref[p, :part, :] = high
        out_ref[p, part : 2 * part, :] = (first - high.astype(f32)).astype(bf16)
        out_ref[p, 2 * part :, :] = jnp.where(equal, sibling[0], sibling[1]).astype(bf16)


def operators_of(ref, rank):
    count, rows, width = ref.shape
    part = rows // 3

    def natural(block):
        value = ref[:, block * part : (block + 1) * part, :].astype(f32)
        halves = [
            value[:, half * part // 2 : (half + 1) * part // 2, :].reshape(-1, width)
            for half in range(2)
        ]
        return jnp.concatenate(halves, axis=0)

    first, rest, second = (natural(block) for block in range(3))
    first = first + rest
    row_level = lax.broadcasted_iota(jnp.int32, (width, width), 0) // rank
    lane_level = lax.broadcasted_iota(jnp.int32, (width, width), 1) // rank
    return first, second, lane_level > row_level


def eliminate_body(terms_ref, operators_ref, out_ref, *, rank):
    columns, width = terms_ref.shape
    count, share, _ = out_ref.shape
    first, _, ahead = operators_of(operators_ref, rank)
    feed = jnp.where(ahead, first, 0.0)
    half = width // 2

    def solve(value, square):
        double = full_dot(square, square)
        value = value - full_dot(value, square)
        return value + full_dot(value, double)

    early = solve(terms_ref[:, :half], feed[:half, :half])
    late = terms_ref[:, half:] - full_dot(early, feed[:half, half:])
    late = solve(late, feed[half:, half:])
    for j in range(count):
        rows = slice(j * share, (j + 1) * share)
        out_ref[j, :, :half] = early[rows, :]
        out_ref[j, :, half:] = late[rows, :]


def sums_body(place_ref, spread_ref, high_ref, out_ref, *, rank):
    low_count, share, width = spread_ref.shape
    high_count, _, high_width = high_ref.shape
    low_width = width - high_width
    low_levels = low_count.bit_length() - 1
    high_levels = high_count.bit_length() - 1
    lane_level = lax.broadcasted_iota(jnp.int32, (share, width), 1) // rank
    tree = node_sums([spread_ref[p] for p in range(low_count)], low_levels)
    blank = jnp.zeros((share, low_width), f32)
    highs = []
    for values in chain_sums([high_ref[p] for p in range(high_count)], place_ref[1], high_levels):
        pick = values[0]
        for level in range(1, high_levels):
            pick = jnp.where(lane_level[:, low_width:] == low_levels + level, values[level], pick)
        highs.append(jnp.concatenate([blank, pick], axis=1))
    for p in range(low_count):
        mine, other = highs
        for level in range(low_levels):
            chosen = lane_level == level
            mine = jnp.where(chosen, tree[level][p >> level], mine)
            other = jnp.where(chosen, tree[level][(p >> level) ^ 1], other)
        out_ref[p, :share, :] = mine
        out_ref[p, share:, :] = other


def weights_body(sums_ref, state_ref, basis_ref, coupling_ref, weights_ref, joined_ref, *, local_levels):
    count, rows, width = sums_ref.shape
    share = rows // 2
    columns = count * share
    rank = coupling_ref.shape[1]
    for j in range(count):
        joined_ref[j * share : (j + 1) * share, :] = sums_ref[j, :share, :]
        joined_ref[columns + j * share : columns + (j + 1) * share, :] = sums_ref[j, share:, :]
    pieces = []
    for level in range(width // rank):
        lanes = slice(level * rank, (level + 1) * rank)
        joined = jnp.concatenate(
            [joined_ref[:columns, lanes], joined_ref[columns:, lanes]], axis=1
        )
        pieces.append(full_dot(joined, coupling_ref[local_levels + level], rows_by_rows))
    mixed = jnp.concatenate(pieces, axis=1)
    update = wide_dot(mixed, basis_ref[local_levels * rank :, :], rows_by_columns)
    weights_ref[...] = (state_ref[...] - update).astype(bf16)


def far_body(joined_ref, operators_ref, test_ref, out_ref, *, rank, factor):
    columns = out_ref.shape[0]
    first, second, ahead = operators_of(operators_ref, rank)
    own = joined_ref[:columns, :]
    sibling = joined_ref[columns:, :]
    far = (
        sibling
        - full_dot(own, jnp.where(ahead, 0.0, first))
        - full_dot(sibling, jnp.where(ahead, 0.0, second))
    )
    out_ref[...] = wide_dot(far, test_ref[...], rows_by_columns) / factor


def mean_body(
    slots_ref, before_ref, mine_ref, after_ref, values_ref, last_ref, far_ref,
    out_ref, window_ref, near_ref, held_ref, arrived, *, leaf_size, factor,
):
    stored = values_ref.shape[0]
    leaf_count = mine_ref.shape[1] // leaf_size
    copies = [
        pltpu.make_async_copy(values_ref.at[slot], held_ref.at[slot], arrived.at[slot])
        for slot in range(stored)
    ]
    for copy in copies:
        copy.start()
    for side, ref in enumerate((before_ref, mine_ref, after_ref)):
        for leaf in range(leaf_count):
            window_ref[side * leaf_count + leaf] = ref[:, leaf * leaf_size : (leaf + 1) * leaf_size]

    def part_of(slot, values):
        return jnp.dot(window_ref[slots_ref[slot]], values, preferred_element_type=f32)

    near_ref[...] = far_ref[...]
    for place in range(last_ref.shape[0]):
        near_ref[...] += part_of(stored + place, last_ref[place])
    for slot in range(stored):
        copies[slot].wait()
        near_ref[...] += part_of(slot, held_ref[slot])
    out_ref[...] = (near_ref[...] * factor).astype(bf16)


def mean_kernel(slots, before, mine, after, values, last, far, factor):
    stored, leaf_size, tests = values.shape
    columns, points = mine.shape

    def body(*refs):
        mean_body(*refs, leaf_size=leaf_size, factor=factor)

    vmem = pl.BlockSpec(memory_space=pltpu.VMEM)
    return pl.pallas_call(
        body,
        out_shape=jax.ShapeDtypeStruct((columns, tests), bf16),
        in_specs=[
            pl.BlockSpec(memory_space=pltpu.SMEM),
            vmem,
            vmem,
            vmem,
            pl.BlockSpec(memory_space=pl.ANY),
            vmem,
            vmem,
        ],
        out_specs=vmem,
        scratch_shapes=[
            pltpu.VMEM((3 * points // leaf_size, columns, leaf_size), bf16),
            pltpu.VMEM((columns, tests), f32),
            pltpu.VMEM(values.shape, bf16),
            pltpu.SemaphoreType.DMA((stored,)),
        ],
        compiler_params=pltpu.CompilerParams(vmem_limit_bytes=24 << 20),
        name="posterior_mean",
    )(
        slots, before, mine, after,
        pltpu.with_memory_space_constraint(values, pltpu.HBM), last, far,
    )


def exchange(value, axes):
    return lax.all_to_all(value, axes, 0, 0)


def gathered(value, axes):
    count = lax.axis_size(axes)
    return exchange(jnp.broadcast_to(value[None], (count,) + value.shape), axes)


def tie(*values):
    return lax.optimization_barrier(values)


def shards(
    targets,
    tree_order,
    leaf_inverse,
    cluster_basis,
    coupling,
    train_coords,
    test_coords,
    test_basis,
    near_leaves,
):
    columns, points = targets.shape
    leaf_count, leaf_size = leaf_inverse.shape[:2]
    all_levels, rank = cluster_basis.shape[:2]
    local_levels = leaf_count.bit_length() - 1
    low_count = lax.axis_size(low_axes)
    high_count = lax.axis_size("z")
    low_levels = low_count.bit_length() - 1
    low = lax.axis_index(low_axes)
    high = lax.axis_index("z")
    panels = low_count * high_count
    width = (all_levels - local_levels) * rank
    low_width = low_levels * rank
    part = width // low_count
    share = columns // low_count
    place = jnp.stack([low, high]).astype(jnp.int32)
    position = high * low_count + low
    basis = cluster_basis.reshape(all_levels * rank, points)
    mixers = coupling[0]
    slot_count = near_leaves.shape[1]
    last_count = slot_count // 4
    stored = slot_count - last_count

    def mixer(*refs):
        mixer_body(*refs, local_levels=local_levels)

    effect = whole_call(
        mixer, jax.ShapeDtypeStruct((low_count, 2 * part, width), f32), "mixer", limit=None
    )(basis, mixers)
    effect, train_coords = tie(effect, train_coords)
    spread = exchange(effect, low_axes)

    def featured(*refs):
        points_body(*refs, scale=3.0 / length_scale**2)

    features = jax.ShapeDtypeStruct((16, points), bf16)
    train_rows, test_rows = whole_call(
        featured, [features] * 2, "points", scratch=[pltpu.VMEM((16, points), f32)]
    )(train_coords, test_coords)
    forward = [(i, i + 1) for i in range(panels - 1)]
    backward = [(i + 1, i) for i in range(panels - 1)]
    train_rows, tree_order = tie(train_rows, tree_order)

    state, terms = whole_call(
        local_body,
        [
            jax.ShapeDtypeStruct((columns, points), f32),
            jax.ShapeDtypeStruct((columns, width), f32),
        ],
        "local",
        limit=None,
    )(targets, tree_order, leaf_inverse, basis, mixers)
    terms, spread = tie(terms, spread)

    slots = near_leaves[0] - (position - 1) * leaf_count
    total = jnp.sum(spread, axis=0).reshape(2, part, width)[:, part // 2 :, low_width:]
    total = total.reshape(part, width - low_width)
    train_rows, total = tie(train_rows, total)
    sides = (
        lax.ppermute(train_rows, panel_axes, forward),
        train_rows,
        lax.ppermute(train_rows, panel_axes, backward),
    )
    high_spread = gathered(total, "z")
    *sides, high_spread = tie(*sides, high_spread)

    def operator(*refs):
        operator_body(*refs, rank=rank)

    operators = whole_call(
        operator, jax.ShapeDtypeStruct((low_count, 3 * part, width), bf16), "operator", 1
    )(place, spread, high_spread)
    late_slots, operators = tie(slots[:stored], operators)
    operators = exchange(operators, low_axes)
    late = distance_kernel(late_slots, sides, test_rows, leaf_size, "near_late", pltpu.HBM)
    late, operators = tie(late, operators)

    def eliminate(*refs):
        eliminate_body(*refs, rank=rank)

    own_terms = whole_call(
        eliminate, jax.ShapeDtypeStruct((low_count, share, width), f32), "eliminate"
    )(terms, operators)
    spread = exchange(own_terms, low_axes)
    high_spread = gathered(jnp.sum(spread, axis=0)[:, low_width:], "z")

    def subtree(*refs):
        sums_body(*refs, rank=rank)

    sums = whole_call(
        subtree, jax.ShapeDtypeStruct((low_count, 2 * share, width), f32), "subtree", 1
    )(place, spread, high_spread)
    sums = exchange(sums, low_axes)

    def weigh(*refs):
        weights_body(*refs, local_levels=local_levels)

    weights, joined = whole_call(
        weigh,
        [
            jax.ShapeDtypeStruct((columns, points), bf16),
            jax.ShapeDtypeStruct((2 * columns, width), f32),
        ],
        "weights",
    )(sums, state, basis, mixers)
    last_slots, weights = tie(slots[stored:], weights)
    last = distance_kernel(
        last_slots, sides, test_rows, leaf_size, "near_last", jax.ShapeDtypeStruct
    )
    before = lax.ppermute(weights, panel_axes, forward)
    after = lax.ppermute(weights, panel_axes, backward)
    factor = 2.0 / math.sqrt(near_leaves.shape[1] * leaf_size)

    def distant(*refs):
        far_body(*refs, rank=rank, factor=factor)

    far = whole_call(distant, jax.ShapeDtypeStruct((columns, points), f32), "far")(
        joined, operators, test_basis.reshape(width, -1)
    )
    return mean_kernel(slots, before, weights, after, late, last, far, factor)


def solution(mesh):
    grp, leaf, sub = (mesh.shape[name] for name in ("grp", "leaf", "sub"))
    split = Mesh(mesh.devices.reshape(grp, leaf // 2, 2, sub), ("grp",) + panel_axes)
    every = ("grp",) + panel_axes
    return jax.shard_map(
        shards,
        mesh=split,
        in_specs=(
            P(None, every),
            P(every, None),
            P(every, None, None),
            P(None, None, every),
            P(every, None, None, None),
            P(None, every),
            P(None, every),
            P(None, None, every),
            P(every, None),
        ),
        out_specs=P(None, every),
        check_vma=False,
    )
```

```python
import math

import jax
import jax.numpy as jnp
from jax import lax
from jax.experimental import pallas as pl
from jax.experimental.pallas import tpu as pltpu
from jax.sharding import Mesh
from jax.sharding import PartitionSpec as P

length_scale = 0.5
highest = lax.Precision.HIGHEST
low_axes = ("core", "sub")
panel_axes = ("z", "core", "sub")
f32 = jnp.float32
bf16 = jnp.bfloat16
rows_by_columns = (((1,), (0,)), ((), ()))
rows_by_rows = (((1,), (1,)), ((), ()))
columns_by_columns = (((0,), (0,)), ((), ()))


def thirds(value):
    high = value.astype(bf16)
    rest = value - high.astype(f32)
    middle = rest.astype(bf16)
    low = (rest - middle.astype(f32)).astype(bf16)
    return high, middle, low


def wide_dot(left, right, dims):
    rows = left.shape[0]
    stacked = jnp.concatenate(thirds(left), axis=0)
    product = lax.dot_general(stacked, right, dims, preferred_element_type=f32)
    return product[:rows] + product[rows : 2 * rows] + product[2 * rows :]


def full_dot(left, right, dims=rows_by_columns):
    return lax.dot_general(left, right, dims, precision=highest, preferred_element_type=f32)


def whole_call(body, out_shape, name, scalars=0, scratch=(), limit=20 << 20):
    def call(*operands):
        specs = [
            pl.BlockSpec(memory_space=pltpu.SMEM if i < scalars else pltpu.VMEM)
            for i in range(len(operands))
        ]
        single = not isinstance(out_shape, (list, tuple))
        out_specs = pl.BlockSpec(memory_space=pltpu.VMEM)
        return pl.pallas_call(
            body,
            out_shape=out_shape,
            in_specs=specs,
            out_specs=out_specs if single else [out_specs] * len(out_shape),
            scratch_shapes=list(scratch),
            name=name,
            compiler_params=pltpu.CompilerParams(vmem_limit_bytes=limit),
        )(*operands)

    return call


def points_body(train_ref, test_ref, left_ref, right_ref, rows_ref, *, scale):
    dims, count = train_ref.shape
    ones = jnp.ones((1, count), f32)
    for ref, out_ref in ((train_ref, left_ref), (test_ref, right_ref)):
        exact = ref[...].astype(f32)
        norms = scale * jnp.sum(exact * exact, axis=0, keepdims=True)
        norms = [piece.astype(f32) for piece in thirds(norms)]
        if out_ref is left_ref:
            rows = [exact[axis : axis + 1] for axis in range(dims)] * 3 + norms + [ones] * 3
        else:
            pieces = [piece.astype(f32) for piece in thirds(-2.0 * scale * exact)]
            rows = [piece[axis : axis + 1] for piece in pieces for axis in range(dims)]
            rows = rows + [ones] * 3 + norms
        rows_ref[...] = jnp.zeros_like(rows_ref)
        for place, row in enumerate(rows):
            rows_ref[place : place + 1, :] = row
        out_ref[...] = rows_ref[...].astype(bf16)


def mixer_body(basis_ref, coupling_ref, out_ref, *, local_levels):
    rank = coupling_ref.shape[1]
    width = basis_ref.shape[0] - local_levels * rank
    points = basis_ref.shape[1]
    basis = basis_ref[local_levels * rank :, :]
    gram = lax.dot_general(basis, basis, rows_by_rows, preferred_element_type=f32)
    level = lax.broadcasted_iota(jnp.int32, (1, width), 1) // rank
    gram = gram * (lax.exp2(-0.5 * level.astype(f32)) / math.sqrt(points))
    piece = out_ref.shape[1] // 4
    for depth in range(width // rank):
        rows = gram[depth * rank : (depth + 1) * rank, :]
        product = full_dot(coupling_ref[local_levels + depth], rows, columns_by_columns)
        upper, group = divmod(depth, width // rank // 2)
        for half in range(2):
            for block in range(rank // piece):
                start = half * rank + block * piece
                row = (2 * half + upper) * piece
                out_ref[group * (rank // piece) + block, row : row + piece, :] = product[
                    start : start + piece, :
                ]


def local_body(targets_ref, order_ref, inverse_ref, basis_ref, coupling_ref, state_ref, terms_ref):
    columns, points = targets_ref.shape
    leaf_count, leaf_size, _ = inverse_ref.shape
    rank = coupling_ref.shape[1]
    local_levels = leaf_count.bit_length() - 1
    place = lax.broadcasted_iota(jnp.int32, (points, leaf_size), 0)
    for leaf in range(leaf_count):
        lanes = slice(leaf * leaf_size, (leaf + 1) * leaf_size)
        chosen = jnp.where(place == order_ref[:, lanes], 1.0, 0.0).astype(bf16)
        block = jnp.dot(targets_ref[...], chosen, preferred_element_type=f32).astype(bf16)
        state_ref[:, lanes] = lax.dot_general(
            block, inverse_ref[leaf], rows_by_rows, preferred_element_type=f32
        )
    for level in range(local_levels):
        child = leaf_size << level
        count = points // child
        mixers = coupling_ref[level]
        bases = [
            basis_ref[level * rank : (level + 1) * rank, c * child : (c + 1) * child]
            for c in range(count)
        ]
        sums = [
            wide_dot(state_ref[:, c * child : (c + 1) * child], bases[c], rows_by_rows)
            / math.sqrt(child)
            for c in range(count)
        ]
        for c in range(count):
            joined = jnp.concatenate([sums[c], sums[c ^ 1]], axis=1)
            mixed = full_dot(joined, mixers, rows_by_rows)
            lanes = slice(c * child, (c + 1) * child)
            state_ref[:, lanes] = state_ref[:, lanes] - wide_dot(mixed, bases[c], rows_by_columns)
    width = terms_ref.shape[1]
    level = lax.broadcasted_iota(jnp.int32, (1, width), 1) // rank
    scale = lax.exp2(-0.5 * level.astype(f32)) / math.sqrt(points)
    terms_ref[...] = (
        wide_dot(state_ref[...], basis_ref[local_levels * rank :, :], rows_by_rows) * scale
    )


def distance_body(
    slots_ref, before_ref, mine_ref, after_ref, test_ref, out_ref, train_ref, *, first
):
    leaf = slots_ref[first + pl.program_id(0)]
    leaf_size = train_ref.shape[1]
    leaf_count = mine_ref.shape[1] // leaf_size
    for side, ref in enumerate((before_ref, mine_ref, after_ref)):

        @pl.when(leaf // leaf_count == side)
        def _(ref=ref):
            start = pl.multiple_of((leaf % leaf_count) * leaf_size, leaf_size)
            train_ref[...] = ref[:, pl.ds(start, leaf_size)]

    train = train_ref[...]
    step = 256
    for start in range(0, test_ref.shape[1], step):
        squared = lax.dot_general(
            train, test_ref[:, start : start + step], columns_by_columns,
            preferred_element_type=f32,
        )
        squared = jnp.maximum(squared, 1e-20)
        scaled = squared * lax.rsqrt(squared)
        out_ref[0, :, start : start + step] = ((1.0 + scaled) * jnp.exp(-scaled)).astype(bf16)


def distance_kernel(slots, first, count, sides, test_features, leaf_size, name, store):
    tests = test_features.shape[1]
    operands = (*sides, test_features)

    def body(*refs):
        distance_body(*refs, first=first)

    return pl.pallas_call(
        body,
        out_shape=store((count, leaf_size, tests), bf16),
        grid_spec=pltpu.PrefetchScalarGridSpec(
            num_scalar_prefetch=1,
            grid=(count,),
            in_specs=[pl.BlockSpec(a.shape, lambda i, s: (0, 0)) for a in operands],
            out_specs=pl.BlockSpec((1, leaf_size, tests), lambda i, s: (i, 0, 0)),
            scratch_shapes=[pltpu.VMEM((sides[0].shape[0], leaf_size), bf16)],
        ),
        compiler_params=pltpu.CompilerParams(vmem_limit_bytes=24 << 20),
        name=name,
    )(slots, *operands)


def node_sums(members, levels):
    sums = [members]
    for _ in range(levels):
        last = sums[-1]
        sums.append([last[i] + last[i + 1] for i in range(0, len(last), 2)])
    return sums


def chain_sums(values, position, levels):
    tree = node_sums(values, levels)
    own, sibling = [], []
    for level in range(levels):
        nodes = tree[level]
        mine = position >> level
        first, second = nodes[0], nodes[1]
        for node in range(2, len(nodes), 2):
            here = (mine >> 1) == (node >> 1)
            first = jnp.where(here, nodes[node], first)
            second = jnp.where(here, nodes[node + 1], second)
        right = (mine & 1) == 1
        own.append(jnp.where(right, second, first))
        sibling.append(jnp.where(right, first, second))
    return own, sibling


def operator_body(place_ref, spread_ref, high_ref, out_ref, *, rank):
    low_count, rows, width = spread_ref.shape
    part = rows // 2
    high_count, _, high_width = high_ref.shape
    low_width = width - high_width
    low_levels = low_count.bit_length() - 1
    high_levels = high_count.bit_length() - 1
    piece = part // 2
    row = lax.broadcasted_iota(jnp.int32, (part, width), 0)
    row_level = place_ref[0] * piece // rank + low_levels * (row // piece)
    lane_level = lax.broadcasted_iota(jnp.int32, (part, width), 1) // rank
    pair_level = jnp.minimum(lane_level, row_level)
    below = lane_level < row_level
    equal = lane_level == row_level
    blank = jnp.zeros((piece, low_width), f32)
    trees = []
    highs = []
    for half in range(2):
        rows_here = slice(half * part, (half + 1) * part)
        trees.append(node_sums([spread_ref[p, rows_here, :] for p in range(low_count)], low_levels))
        own, sibling = chain_sums(
            [high_ref[p, half * piece : (half + 1) * piece, :] for p in range(high_count)],
            place_ref[1],
            high_levels,
        )
        picks = []
        for values in (own, sibling):
            pick = values[0]
            for level in range(1, high_levels):
                pick = jnp.where(
                    pair_level[piece:, low_width:] == low_levels + level, values[level], pick
                )
            pick = jnp.concatenate([blank, pick], axis=1)
            picks.append(jnp.concatenate([jnp.zeros_like(pick), pick], axis=0))
        highs.append(picks)
    for p in range(low_count):
        own, sibling = [], []
        for half in range(2):
            mine, other = highs[half]
            for level in range(low_levels):
                chosen = pair_level == level
                mine = jnp.where(chosen, trees[half][level][p >> level], mine)
                other = jnp.where(chosen, trees[half][level][(p >> level) ^ 1], other)
            own.append(mine)
            sibling.append(other)
        ahead = own[0] + sibling[1]
        first = jnp.where(below, sibling[0], jnp.where(equal, sibling[1], ahead))
        high = first.astype(bf16)
        out_ref[p, :part, :] = high
        out_ref[p, part : 2 * part, :] = (first - high.astype(f32)).astype(bf16)
        out_ref[p, 2 * part :, :] = jnp.where(equal, sibling[0], sibling[1]).astype(bf16)


def operators_of(ref, rank):
    count, rows, width = ref.shape
    part = rows // 3

    def natural(block):
        value = ref[:, block * part : (block + 1) * part, :].astype(f32)
        halves = [
            value[:, half * part // 2 : (half + 1) * part // 2, :].reshape(-1, width)
            for half in range(2)
        ]
        return jnp.concatenate(halves, axis=0)

    first, rest, second = (natural(block) for block in range(3))
    first = first + rest
    row_level = lax.broadcasted_iota(jnp.int32, (width, width), 0) // rank
    lane_level = lax.broadcasted_iota(jnp.int32, (width, width), 1) // rank
    return first, second, lane_level > row_level


def eliminate_body(terms_ref, operators_ref, out_ref, *, rank):
    columns, width = terms_ref.shape
    count, share, _ = out_ref.shape
    first, _, ahead = operators_of(operators_ref, rank)
    feed = jnp.where(ahead, first, 0.0)
    half = width // 2

    def solve(value, square):
        double = full_dot(square, square)
        value = value - full_dot(value, square)
        return value + full_dot(value, double)

    early = solve(terms_ref[:, :half], feed[:half, :half])
    late = terms_ref[:, half:] - full_dot(early, feed[:half, half:])
    late = solve(late, feed[half:, half:])
    for j in range(count):
        rows = slice(j * share, (j + 1) * share)
        out_ref[j, :, :half] = early[rows, :]
        out_ref[j, :, half:] = late[rows, :]


def sums_body(place_ref, spread_ref, high_ref, out_ref, *, rank):
    low_count, share, width = spread_ref.shape
    high_count, _, high_width = high_ref.shape
    low_width = width - high_width
    low_levels = low_count.bit_length() - 1
    high_levels = high_count.bit_length() - 1
    lane_level = lax.broadcasted_iota(jnp.int32, (share, width), 1) // rank
    tree = node_sums([spread_ref[p] for p in range(low_count)], low_levels)
    blank = jnp.zeros((share, low_width), f32)
    highs = []
    for values in chain_sums([high_ref[p] for p in range(high_count)], place_ref[1], high_levels):
        pick = values[0]
        for level in range(1, high_levels):
            pick = jnp.where(lane_level[:, low_width:] == low_levels + level, values[level], pick)
        highs.append(jnp.concatenate([blank, pick], axis=1))
    for p in range(low_count):
        mine, other = highs
        for level in range(low_levels):
            chosen = lane_level == level
            mine = jnp.where(chosen, tree[level][p >> level], mine)
            other = jnp.where(chosen, tree[level][(p >> level) ^ 1], other)
        out_ref[p, :share, :] = mine
        out_ref[p, share:, :] = other


def weights_body(sums_ref, state_ref, basis_ref, coupling_ref, weights_ref, joined_ref, *, local_levels):
    count, rows, width = sums_ref.shape
    share = rows // 2
    columns = count * share
    rank = coupling_ref.shape[1]
    for j in range(count):
        joined_ref[j * share : (j + 1) * share, :] = sums_ref[j, :share, :]
        joined_ref[columns + j * share : columns + (j + 1) * share, :] = sums_ref[j, share:, :]
    pieces = []
    for level in range(width // rank):
        lanes = slice(level * rank, (level + 1) * rank)
        joined = jnp.concatenate(
            [joined_ref[:columns, lanes], joined_ref[columns:, lanes]], axis=1
        )
        pieces.append(full_dot(joined, coupling_ref[local_levels + level], rows_by_rows))
    mixed = jnp.concatenate(pieces, axis=1)
    update = wide_dot(mixed, basis_ref[local_levels * rank :, :], rows_by_columns)
    weights_ref[...] = (state_ref[...] - update).astype(bf16)


def far_body(joined_ref, operators_ref, test_ref, out_ref, *, rank, factor):
    columns = out_ref.shape[0]
    first, second, ahead = operators_of(operators_ref, rank)
    own = joined_ref[:columns, :]
    sibling = joined_ref[columns:, :]
    far = (
        sibling
        - full_dot(own, jnp.where(ahead, 0.0, first))
        - full_dot(sibling, jnp.where(ahead, 0.0, second))
    )
    out_ref[...] = wide_dot(far, test_ref[...], rows_by_columns) / factor


def mean_body(
    slots_ref, before_ref, mine_ref, after_ref, values_ref, last_ref, far_ref,
    out_ref, window_ref, near_ref, held_ref, arrived, *, leaf_size, factor,
):
    stored = values_ref.shape[0]
    leaf_count = mine_ref.shape[1] // leaf_size
    copies = [
        pltpu.make_async_copy(values_ref.at[slot], held_ref.at[slot], arrived.at[slot])
        for slot in range(stored)
    ]
    for copy in copies:
        copy.start()
    for side, ref in enumerate((before_ref, mine_ref, after_ref)):
        for leaf in range(leaf_count):
            window_ref[side * leaf_count + leaf] = ref[:, leaf * leaf_size : (leaf + 1) * leaf_size]

    def part_of(slot, values):
        return jnp.dot(window_ref[slots_ref[slot]], values, preferred_element_type=f32)

    near_ref[...] = far_ref[...]
    for place in range(last_ref.shape[0]):
        near_ref[...] += part_of(stored + place, last_ref[place])
    for slot in range(stored):
        copies[slot].wait()
        near_ref[...] += part_of(slot, held_ref[slot])
    out_ref[...] = (near_ref[...] * factor).astype(bf16)


def mean_kernel(slots, before, mine, after, values, last, far, factor):
    stored, leaf_size, tests = values.shape
    columns, points = mine.shape

    def body(*refs):
        mean_body(*refs, leaf_size=leaf_size, factor=factor)

    vmem = pl.BlockSpec(memory_space=pltpu.VMEM)
    return pl.pallas_call(
        body,
        out_shape=jax.ShapeDtypeStruct((columns, tests), bf16),
        in_specs=[
            pl.BlockSpec(memory_space=pltpu.SMEM),
            vmem,
            vmem,
            vmem,
            pl.BlockSpec(memory_space=pl.ANY),
            vmem,
            vmem,
        ],
        out_specs=vmem,
        scratch_shapes=[
            pltpu.VMEM((3 * points // leaf_size, columns, leaf_size), bf16),
            pltpu.VMEM((columns, tests), f32),
            pltpu.VMEM(values.shape, bf16),
            pltpu.SemaphoreType.DMA((stored,)),
        ],
        compiler_params=pltpu.CompilerParams(vmem_limit_bytes=24 << 20),
        name="posterior_mean",
    )(
        slots, before, mine, after,
        pltpu.with_memory_space_constraint(values, pltpu.HBM), last, far,
    )


def exchange(value, axes):
    return lax.all_to_all(value, axes, 0, 0)


def gathered(value, axes):
    count = lax.axis_size(axes)
    return exchange(jnp.broadcast_to(value[None], (count,) + value.shape), axes)


def tie(*values):
    return lax.optimization_barrier(values)


def shards(
    targets,
    tree_order,
    leaf_inverse,
    cluster_basis,
    coupling,
    train_coords,
    test_coords,
    test_basis,
    near_leaves,
):
    columns, points = targets.shape
    leaf_count, leaf_size = leaf_inverse.shape[:2]
    all_levels, rank = cluster_basis.shape[:2]
    local_levels = leaf_count.bit_length() - 1
    low_count = lax.axis_size(low_axes)
    high_count = lax.axis_size("z")
    low_levels = low_count.bit_length() - 1
    low = lax.axis_index(low_axes)
    high = lax.axis_index("z")
    panels = low_count * high_count
    width = (all_levels - local_levels) * rank
    low_width = low_levels * rank
    part = width // low_count
    share = columns // low_count
    place = jnp.stack([low, high]).astype(jnp.int32)
    position = high * low_count + low
    basis = cluster_basis.reshape(all_levels * rank, points)
    mixers = coupling[0]
    slot_count = near_leaves.shape[1]
    last_count = slot_count // 4
    stored = slot_count - last_count

    def mixer(*refs):
        mixer_body(*refs, local_levels=local_levels)

    effect = whole_call(
        mixer, jax.ShapeDtypeStruct((low_count, 2 * part, width), f32), "mixer", limit=None
    )(basis, mixers)
    effect, train_coords = tie(effect, train_coords)
    spread = exchange(effect, low_axes)

    def featured(*refs):
        points_body(*refs, scale=3.0 / length_scale**2)

    features = jax.ShapeDtypeStruct((16, points), bf16)
    train_rows, test_rows = whole_call(
        featured, [features] * 2, "points", scratch=[pltpu.VMEM((16, points), f32)]
    )(train_coords, test_coords)
    forward = [(i, i + 1) for i in range(panels - 1)]
    backward = [(i + 1, i) for i in range(panels - 1)]
    train_rows, tree_order = tie(train_rows, tree_order)

    state, terms = whole_call(
        local_body,
        [
            jax.ShapeDtypeStruct((columns, points), f32),
            jax.ShapeDtypeStruct((columns, width), f32),
        ],
        "local",
        limit=None,
    )(targets, tree_order, leaf_inverse, basis, mixers)
    terms, spread = tie(terms, spread)

    slots = near_leaves[0] - (position - 1) * leaf_count
    total = jnp.sum(spread, axis=0).reshape(2, part, width)[:, part // 2 :, low_width:]
    total = total.reshape(part, width - low_width)
    train_rows, total = tie(train_rows, total)
    sides = (
        lax.ppermute(train_rows, panel_axes, forward),
        train_rows,
        lax.ppermute(train_rows, panel_axes, backward),
    )
    high_spread = gathered(total, "z")
    *sides, high_spread = tie(*sides, high_spread)

    def operator(*refs):
        operator_body(*refs, rank=rank)

    operators = whole_call(
        operator, jax.ShapeDtypeStruct((low_count, 3 * part, width), bf16), "operator", 1
    )(place, spread, high_spread)
    late_rows, operators = tie(test_rows, operators)
    operators = exchange(operators, low_axes)
    late = distance_kernel(
        slots, 0, stored, sides, late_rows, leaf_size, "near_late", pltpu.HBM
    )
    late, operators = tie(late, operators)

    def eliminate(*refs):
        eliminate_body(*refs, rank=rank)

    own_terms = whole_call(
        eliminate, jax.ShapeDtypeStruct((low_count, share, width), f32), "eliminate"
    )(terms, operators)
    spread = exchange(own_terms, low_axes)
    high_spread = gathered(jnp.sum(spread, axis=0)[:, low_width:], "z")

    def subtree(*refs):
        sums_body(*refs, rank=rank)

    sums = whole_call(
        subtree, jax.ShapeDtypeStruct((low_count, 2 * share, width), f32), "subtree", 1
    )(place, spread, high_spread)
    sums = exchange(sums, low_axes)

    def weigh(*refs):
        weights_body(*refs, local_levels=local_levels)

    weights, joined = whole_call(
        weigh,
        [
            jax.ShapeDtypeStruct((columns, points), bf16),
            jax.ShapeDtypeStruct((2 * columns, width), f32),
        ],
        "weights",
    )(sums, state, basis, mixers)
    last_rows, weights = tie(test_rows, weights)
    last = distance_kernel(
        slots, stored, last_count, sides, last_rows, leaf_size, "near_last", jax.ShapeDtypeStruct
    )
    before = lax.ppermute(weights, panel_axes, forward)
    after = lax.ppermute(weights, panel_axes, backward)
    factor = 2.0 / math.sqrt(near_leaves.shape[1] * leaf_size)

    def distant(*refs):
        far_body(*refs, rank=rank, factor=factor)

    far = whole_call(distant, jax.ShapeDtypeStruct((columns, points), f32), "far")(
        joined, operators, test_basis.reshape(width, -1)
    )
    return mean_kernel(slots, before, weights, after, late, last, far, factor)


def solution(mesh):
    grp, leaf, sub = (mesh.shape[name] for name in ("grp", "leaf", "sub"))
    split = Mesh(mesh.devices.reshape(grp, leaf // 2, 2, sub), ("grp",) + panel_axes)
    every = ("grp",) + panel_axes
    return jax.shard_map(
        shards,
        mesh=split,
        in_specs=(
            P(None, every),
            P(every, None),
            P(every, None, None),
            P(None, None, every),
            P(every, None, None, None),
            P(None, every),
            P(None, every),
            P(None, None, every),
            P(every, None),
        ),
        out_specs=P(None, every),
        check_vma=False,
    )
```
